128 devices in a mesh: ta: 64 (over y, x, z), gz: 2 (over core).
Axes of the slice: x: 4, y: 4, z: 4, core: 2. Of those that a mesh axis runs over, the one named last changes fastest.
Arguments:
- propagator: float32 [2, 12, 12, 64, 13824], P(None, None, None, 'ta', 'gz'), may hold values from -6 to 6
- backward: float32 [2, 12, 12, 64, 13824], P(None, None, None, 'ta', 'gz'), may hold values from -6 to 6
- sink_time: int32 [1], replicated, may hold values from 0 to 63
- source_position: int32 [3], replicated, may hold values from 0 to 23
- momenta: int32 [27, 3], replicated, may hold values from -3 to 3
- gamma_table: int32 [16], replicated, may hold values from 0 to 15, each once
Outputs:
- correlator: float32 [2, 64, 16, 27], P(None, 'ta', 'gz')
The draws below stay inside these ranges and needn't reach their ends.
Inputs may be any that keep to these rules, and one draw needn't show every extreme that they name: `gamma_table`: each of 0 to 15 appears exactly once.
All inputs are finite; a program needn't handle non-finite values.
Results may differ from the reference program's by a relative error of at most 0.00007.
Values sent between devices are 32-bit elements; how exact they have to be, the bound alone decides.
A program may use at most 192 MiB of HBM per device.

```python
import math
import jax
import jax.numpy as jnp
import numpy as np
from jax import lax

L = 24
NG = 16
NP = 27
T_SIZE = 64
V3 = 13824


def place_ends(drawn, stream_key, smallest, largest):
    shape = drawn.shape
    place = [jax.random.randint(jax.random.fold_in(stream_key, axis), (), 0, shape[axis]) for axis in range(len(shape))]
    drawn = drawn.at[tuple(place)].set(smallest)
    longest = shape.index(max(shape))
    place[longest] = (place[longest] + 1) % shape[longest]
    return drawn.at[tuple(place)].set(largest)


def steps_of(rng, extent, cuts, low, top_value):
    loudness, own = 1.0, jax.random.fold_in(rng, 6)
    for position, shards_of in cuts:
        heights = jnp.exp(jax.random.uniform(jax.random.fold_in(own, position), (shards_of,), jnp.float32, low / len(cuts), top_value / len(cuts)))
        loudness = loudness * jnp.repeat(heights, extent[position] // shards_of).reshape([-1 if axis == position else 1 for axis in range(len(extent))])
    return loudness


def scatter_about(own_key, shape, scale, most, shards=(), kind=jnp.bfloat16):
    gain = steps_of(own_key, shape, shards, -0.22, 0.18) if shards else 1.0
    values = jax.random.normal(own_key, shape, jnp.float32) * scale * gain
    return jnp.minimum(jnp.maximum(values, -most), most).astype(kind)


def setup_inputs(seed: int = 0) -> dict:
    seeds = jax.random.split(jax.random.key(seed), 7)
    return {
        "propagator": scatter_about(seeds[0], (2, 12, 12, T_SIZE, V3), 1.0, 6.0, ((3, 64), (4, 2)), jnp.float32),
        "backward": scatter_about(seeds[1], (2, 12, 12, T_SIZE, V3), 1.0, 6.0, ((3, 64), (4, 2)), jnp.float32),
        "sink_time": jax.random.randint(seeds[2], (1,), 0, T_SIZE).astype(jnp.int32),
        "source_position": jax.random.randint(seeds[3], (3,), 0, L).astype(jnp.int32),
        "momenta": place_ends(jax.random.randint(seeds[4], (NP, 3), -3, 4), jax.random.fold_in(seeds[4], 1), -3, 3).astype(jnp.int32),
        "gamma_table": jax.random.permutation(seeds[5], NG).astype(jnp.int32),
    }


def gamma_tables():
    paulis = [np.eye(2), np.array([[0.0, 1.0], [1.0, 0.0]]), np.array([[0.0, -1j], [1j, 0.0]]), np.array([[1.0, 0.0], [0.0, -1.0]])]
    matrices = np.stack([np.kron(paulis[number // 4], paulis[number % 4]) for number in range(16)])
    return np.stack([matrices.real, matrices.imag]).astype(np.float32)

def complex_product(einsum_form, left_term, right_term):

    def product(first_op, second_op):
        return jnp.einsum(einsum_form, first_op, second_op, precision=lax.Precision.HIGHEST)
    real_part = product(left_term[0], right_term[0]) - product(left_term[1], right_term[1])
    imag_part = product(left_term[0], right_term[1]) + product(left_term[1], right_term[0])
    return jnp.stack([real_part, imag_part])

def complex_reduce(left_term, right_term, reduce_axis):
    real_part = lax.optimization_barrier(jnp.sum(left_term[0] * right_term[0] - left_term[1] * right_term[1], axis=reduce_axis))
    imag_part = lax.optimization_barrier(jnp.sum(left_term[0] * right_term[1] + left_term[1] * right_term[0], axis=reduce_axis))
    return jnp.stack([real_part, imag_part])

def conjugate(values):
    return jnp.stack([values[0], -values[1]])

def source_field(sink_slice):
    return 0.125 * complex_reduce(sink_slice[:, :, None, :, :], sink_slice[:, None, :, :, :], 2)

def phase_table(site_index, source_position, momenta):
    zplane = site_index // (L * L)
    xline = site_index // L % L
    yline = site_index % L
    wave = momenta[:, 0:1] * (xline[None, :] - source_position[0]) + momenta[:, 1:2] * (yline[None, :] - source_position[1]) + momenta[:, 2:3] * (zplane[None, :] - source_position[2])
    wave = jnp.mod(wave, L)
    angle_value = wave.astype(jnp.float32) * (2.0 * math.pi / L)
    return jnp.stack([jnp.cos(angle_value), -jnp.sin(angle_value)])

def slice_correlator(forward, back_field, sink_field, phases, gammas):
    site_count = forward.shape[-1]
    bound = complex_reduce(back_field[:, :, :, None, :], sink_field[:, None, :, :, :], 1)
    forward_split = forward.reshape(2, 4, 36, site_count)
    bound_split = conjugate(bound).reshape(2, 4, 36, site_count)
    spin_block = complex_reduce(forward_split[:, :, None, :, :], bound_split[:, None, :, :, :], 2)
    gamma_flat = jnp.transpose(gammas, (0, 1, 3, 2)).reshape(2, 16, 16)
    currents = complex_product('gb,bs->gs', gamma_flat, spin_block.reshape(2, 16, site_count))
    scale_factor = 1.0 / (72.0 * math.sqrt(L * L * L))
    return scale_factor * complex_product('gs,ps->gp', currents, phases)

def select_currents(gamma_table, values):
    onehot = (gamma_table[:, None] == jnp.arange(NG, dtype=jnp.int32)[None, :]).astype(jnp.float32)
    return jnp.einsum('cg,xgp->xcp', onehot, values, precision=lax.Precision.HIGHEST)

def reference(propagator, backward, sink_time, source_position, momenta, gamma_table):
    gammas = jnp.asarray(gamma_tables())
    sink_slice = lax.dynamic_index_in_dim(propagator, sink_time[0], 3, keepdims=False)
    sink_field = source_field(sink_slice)
    phases = phase_table(jnp.arange(L * L * L, dtype=jnp.int32), source_position, momenta)

    def one_slice(slice_index):
        forward = lax.dynamic_index_in_dim(propagator, slice_index, 3, keepdims=False)
        back_field = lax.dynamic_index_in_dim(backward, slice_index, 3, keepdims=False)
        return select_currents(gamma_table, slice_correlator(forward, back_field, sink_field, phases, gammas))
    stacked = lax.map(one_slice, jnp.arange(T_SIZE, dtype=jnp.int32))
    return jnp.transpose(stacked, (1, 0, 2, 3))
```

```python
import functools
import itertools
import math

import jax
import jax.numpy as jnp
import numpy as np
from jax import lax
from jax.experimental import pallas as pl
from jax.experimental.pallas import tpu as pltpu
from jax.sharding import PartitionSpec as P

L = 24
NG = 16
NP = 27
CHUNKS = 7
LAG = 6
PACKETS = 4 * CHUNKS
DEPTH = 7
SLOTS = PACKETS + DEPTH * LAG
SENDS = SLOTS - LAG
FIRST = DEPTH * LAG + 4
END = FIRST + PACKETS
OUT_RING = 4
SEM_RING = 16
STEPS = ((1, 0, 0), (-1, 0, 0), (0, 1, 0), (0, -1, 0), (0, 0, 1), (0, 0, -1))
TREE_STEPS = (0, 3, 4, 1, 2, 5)
MESH = pl.DeviceIdType.MESH
F32 = jnp.float32


def moved(v, step, sign=1):
    return tuple((a + sign * b) % 4 for a, b in zip(v, step))


def turned(v):
    return tuple((-c) % 4 for c in (v[2], v[0], v[1]))


def turned_step(d):
    return tuple(-c for c in (d[2], d[0], d[1]))


@functools.cache
def tree_words():
    nodes = list(itertools.product(range(4), repeat=3))
    root, child = (0, 0, 0), (1, 0, 0)

    def level(v):
        return sum(min((a - b) % 4, (b - a) % 4) for a, b in zip(v, child))

    def orbit(tail, step):
        while step != (1, 0, 0):
            tail, step = turned(tail), turned_step(step)
        return tail

    taken = orbit(root, (1, 0, 0))
    options = {
        v: [
            (orbit(moved(v, d, -1), d), d)
            for d in STEPS
            if moved(v, d, -1) != root and level(moved(v, d, -1)) < level(v)
        ]
        for v in nodes
        if v not in (root, child)
    }
    match = {}

    def augment(v, seen):
        for key, d in options[v]:
            if key == taken or key in seen:
                continue
            seen.add(key)
            if key not in match or augment(match[key][0], seen):
                match[key] = (v, d)
                return True
        return False

    for v in options:
        assert augment(v, set())
    into = {child: (1, 0, 0)}
    for v, d in match.values():
        into[v] = d
    depth = {root: 0}

    def depth_of(v):
        if v not in depth:
            depth[v] = depth_of(moved(v, into[v], -1)) + 1
        return depth[v]

    edges = [(v, d) for v, d in into.items()]
    depths = {v: depth_of(v) for v in nodes}
    words = np.zeros((3, 64), np.int32)

    def number(v):
        return (v[0] * 4 + v[1]) * 4 + v[2]

    seen_edges = set()
    for k in range(6):
        assert STEPS.index([d for v, d in edges if moved(v, d, -1) == root][0]) == TREE_STEPS[k]
        for v, d in edges:
            n, j = number(v), STEPS.index(d)
            tail = number(moved(v, d, -1))
            assert (tail, j) not in seen_edges
            seen_edges.add((tail, j))
            words[0, n] |= j << (3 * k)
            words[1, tail] |= k << (3 * j)
        for v, n_hops in depths.items():
            assert n_hops <= DEPTH
            words[2, number(v)] |= n_hops << (3 * k)
        edges = [(turned(v), turned_step(d)) for v, d in edges]
        depths = {turned(v): n_hops for v, n_hops in depths.items()}
    return words.reshape(-1)


def source_pairs():
    return [(i, j) for i in range(12) for j in range(i, 12)]


PAIRS = source_pairs()
PAIR_NUMBER = {p: n for n, p in enumerate(PAIRS)}


def pair_number(i, j):
    return PAIR_NUMBER[(min(i, j), max(i, j))]


def kernel(
    prop, back, words, sink, origin, momenta, gtab, out,
    sv, hv, own, inbox, stream, outbox, sig, hsum, ssum, macc, kbuf, ph_hi, ph_lo,
    mom, acc, cbuf, ex, rx,
    s_sem, h_sem, send_sem, recv_sem, ex_send, ex_recv,
):
    ta = lax.axis_index("ta")
    gz = lax.axis_index("gz")
    cy, cx, cz = ta // 16, (ta // 4) % 4, ta % 4

    def load(src, dst, sem, c):
        sites = 1024 if c < CHUNKS - 1 else 768
        return pltpu.make_async_copy(
            src.at[:, :, :, :, pl.ds(1024 * c, sites)],
            dst.at[c, :, :, :, :, pl.ds(0, sites)],
            sem.at[c],
        )

    for c in range(CHUNKS):
        load(prop, sv, s_sem, c).start()
    for c in range(CHUNKS):
        load(back, hv, h_sem, c).start()

    def neighbour(d):
        x, y, z = STEPS[d]
        return ((cy + y + 4) % 4 * 4 + (cx + x + 4) % 4) * 4 + (cz + z + 4) % 4

    barrier = pltpu.get_barrier_semaphore()
    for d in range(6):
        pl.semaphore_signal(barrier, inc=1, device_id=(neighbour(d), gz), device_id_type=MESH)
    pl.semaphore_signal(barrier, inc=1, device_id=(ta, 1 - gz), device_id_type=MESH)

    root = sink[0]
    rel_x = (cx - root // 4 % 4 + 4) % 4
    rel_y = (cy - root // 16 + 4) % 4
    rel_z = (cz - root % 4 + 4) % 4
    rel = (rel_x * 4 + rel_y) * 4 + rel_z
    is_root = rel == 0
    into_word, from_word, depth_word = words[rel], words[64 + rel], words[128 + rel]
    into = [(into_word >> (3 * k)) & 7 for k in range(6)]
    out_of = [(from_word >> (3 * d)) & 7 for d in range(6)]
    base = [((depth_word >> (3 * k)) & 7) * (13 * LAG // 2) for k in range(6)]

    def source(c, part):
        lo, hi = ((0, 4), (4, 7), (7, 10), (10, 13))[part]
        for k in range(6):
            for n in range(lo, hi):
                i, j = PAIRS[13 * k + n]
                re = im = None
                for m in range(12):
                    a, b = sv[c, 0, i, m], sv[c, 1, i, m]
                    if i == j:
                        r, q = a * a - b * b, a * b
                        q = q + q
                    else:
                        e, f = sv[c, 0, j, m], sv[c, 1, j, m]
                        r, q = a * e - b * f, a * f + b * e
                    re = r if re is None else re + r
                    im = q if im is None else im + q
                own[c, k, 2 * n] = re
                own[c, k, 2 * n + 1] = im

    def message(parity, s, d):
        tiles = 7 - parity
        return pltpu.make_async_remote_copy(
            src_ref=outbox.at[s % OUT_RING, d, pl.ds(0, tiles)],
            dst_ref=inbox.at[s + LAG, d, pl.ds(0, tiles)],
            send_sem=send_sem.at[s % OUT_RING, d],
            recv_sem=recv_sem.at[s % SEM_RING, d],
            device_id=(neighbour(d), gz),
            device_id_type=MESH,
        )

    def chosen(s, k, i):
        best = inbox[s, 5, i]
        for d in range(5):
            best = jnp.where(into[k] == d, inbox[s, d, i], best)
        return best

    def relay(s, parity):
        tiles = 7 - parity
        flat = s // 2 * 13 + 7 * parity
        c, u = s // 4, s % 4
        first = u // 2 * 13 + 7 * parity

        @pl.when(s >= LAG)
        def _():
            for d in range(6):
                message(parity, s - LAG, d).wait_recv()

        @pl.when(s < LAG)
        def _():
            for k in range(6):
                for i in range(tiles):
                    stream[k, flat + i] = own[c, k, first + i]

        @pl.when((s >= LAG) & (s < PACKETS))
        def _():
            for i in range(tiles):
                for k in range(6):
                    stream[k, flat + i] = jnp.where(is_root, own[c, k, first + i], chosen(s, k, i))

        @pl.when(s >= PACKETS)
        def _():
            for i in range(tiles):
                for k in range(6):
                    stream[k, flat + i] = chosen(s, k, i)

        @pl.when(s < SENDS)
        def _():
            @pl.when(s >= OUT_RING)
            def _():
                for d in range(6):
                    message(parity, s - OUT_RING, d).wait_send()

            for d in range(6):
                k = jnp.where(is_root, TREE_STEPS.index(d), out_of[d])
                for i in range(tiles):
                    outbox[s % OUT_RING, d, i] = stream[k, flat + i]
            for d in range(6):
                message(parity, s, d).start()

    def phases(c):
        lane = lax.broadcasted_iota(jnp.int32, (32, 128), 1).astype(F32)
        px, py, pz = mom[0], mom[1], mom[2]
        start = (gz * 6912 + c * 1024).astype(F32)
        for pair in range(4):
            for half in range(2):
                site = lane + (start + (256.0 * pair + 128.0 * half))
                z = jnp.floor((site + 0.5) * (1.0 / 576.0))
                rest = site - z * 576.0
                x = jnp.floor((rest + 0.5) * (1.0 / 24.0))
                y = rest - x * 24.0
                wave = px * (x - ox) + py * (y - oy) + pz * (z - oz)
                wave = wave - 24.0 * jnp.floor((wave + 0.5) * (1.0 / 24.0))
                angle = wave * (2.0 * math.pi / L)
                for row, value in ((0, jnp.cos(angle)), (32, -jnp.sin(angle))):
                    hi = value.astype(jnp.bfloat16)
                    at = (c, pair, pl.ds(row, 32), pl.ds(128 * half, 128))
                    ph_hi[at] = hi
                    ph_lo[at] = (value - hi.astype(F32)).astype(jnp.bfloat16)

    ox, oy, oz = (origin[i].astype(F32) for i in range(3))

    def unpack(c):
        for k in range(6):
            for n in range(13):
                at = base[k] + c * 26 + 2 * n
                re, im = stream[k, at], stream[k, at + 1]
                sig[0, 13 * k + n] = re
                sig[1, 13 * k + n] = im - re
                sig[2, 13 * k + n] = im + re
        for i in range(12):
            for m in range(12):
                ssum[i, m] = sv[c, 0, i, m] + sv[c, 1, i, m]

    def contract(c, al):
        for a in range(3):
            for m in range(12):
                hsum[a, m] = hv[c, 0, 3 * al + a, m] + hv[c, 1, 3 * al + a, m]
        total = [[None] * 3 for _ in range(4)]

        def plus(x, y):
            return y if x is None else x + y

        for block in range(4):
            columns = range(3 * block, 3 * block + 3)
            part = {(a, m): [None] * 3 for a in range(3) for m in columns}
            for k in range(12):
                left = [
                    (hsum[a, k], hv[c, 0, 3 * al + a, k], hv[c, 1, 3 * al + a, k])
                    for a in range(3)
                ]
                for m in columns:
                    n = pair_number(k, m)
                    right = (sig[0, n], sig[1, n], sig[2, n])
                    for a in range(3):
                        for t in range(3):
                            part[a, m][t] = plus(part[a, m][t], left[a][t] * right[t])
            for a in range(3):
                for m in columns:
                    k1, k2, k3 = part[a, m]
                    br, bi = k1 - k3, k1 + k2
                    bound = (br, br + bi, br - bi)
                    for be in range(4):
                        row = 3 * be + a
                        forward = (ssum[row, m], sv[c, 0, row, m], sv[c, 1, row, m])
                        for t in range(3):
                            total[be][t] = plus(total[be][t], forward[t] * bound[t])
        for be in range(4):
            macc[0, be, al] = total[be][0] - total[be][2]
            macc[1, be, al] = total[be][0] - total[be][1]

    def add(p, q):
        return (p[0] + q[0], p[1] + q[1])

    def sub(p, q):
        return (p[0] - q[0], p[1] - q[1])

    def pauli(m):
        d = sub(m[0][1], m[1][0])
        return [add(m[0][0], m[1][1]), add(m[1][0], m[0][1]), (-d[1], d[0]), sub(m[0][0], m[1][1])]

    def project(c):
        inner = [
            [
                pauli(
                    [
                        [
                            (macc[0, 2 * b1 + b0, 2 * a1 + a0], macc[1, 2 * b1 + b0, 2 * a1 + a0])
                            for a0 in range(2)
                        ]
                        for b0 in range(2)
                    ]
                )
                for a1 in range(2)
            ]
            for b1 in range(2)
        ]
        site = lax.broadcasted_iota(jnp.int32, (1, 1024), 1)
        valid = (site < 768) | (c < CHUNKS - 1)
        for low in range(4):
            outer = pauli([[inner[b1][a1][low] for a1 in range(2)] for b1 in range(2)])
            for high in range(4):
                n = 4 * high + low
                for part in range(2):
                    kbuf[pl.ds(16 * part + n, 1), :] = jnp.where(valid, outer[high][part], 0.0)
        result = acc[...]
        dims = (((1,), (1,)), ((), ()))
        for pair in range(4):
            left = kbuf[:, pl.ds(256 * pair, 256)]
            hi = left.astype(jnp.bfloat16)
            lo = (left - hi.astype(F32)).astype(jnp.bfloat16)
            for x, y in ((hi, ph_hi), (lo, ph_hi), (hi, ph_lo)):
                result = result + lax.dot_general(
                    x, y[c, pair], dims, preferred_element_type=F32
                )
        acc[...] = result

    acc[...] = jnp.zeros_like(acc)
    load(prop, sv, s_sem, 0).wait()
    source(0, 0)
    pl.semaphore_wait(barrier, 7)

    def slot(s, carry):
        for parity in range(2):
            @pl.when((s % 2 == parity) & (s < SLOTS))
            def _(parity=parity):
                relay(s, parity)

        for u in range(4):
            @pl.when((s % 4 == u) & (s + 1 < PACKETS))
            def _(u=u):
                if u == 3:
                    for c in range(1, CHUNKS):
                        @pl.when(s + 1 == 4 * c)
                        def _(c=c):
                            load(prop, sv, s_sem, c).wait()
                source((s + 1) // 4, (u + 1) % 4)

        @pl.when(s == PACKETS)
        def _():
            mom[...] = jnp.zeros_like(mom)
            for p in range(NP):
                for i in range(3):
                    mom[i, pl.ds(p, 1), :] = jnp.full((1, 128), momenta[i, p], jnp.int32).astype(F32)
            for c in range(CHUNKS):
                load(back, hv, h_sem, c).wait()

        @pl.when((s > PACKETS) & (s <= PACKETS + CHUNKS))
        def _():
            phases(s - PACKETS - 1)

        @pl.when(s >= FIRST)
        def _():
            t = s - FIRST
            c, al = t // 4, t % 4

            @pl.when(al == 0)
            def _():
                unpack(c)

            contract(c, al)

            @pl.when(al == 3)
            def _():
                project(c)

        return carry

    lax.fori_loop(0, END, slot, 0)
    for s in range(SENDS - OUT_RING, SENDS):
        for d in range(6):
            message(s % 2, s, d).wait_send()

    scale = 0.125 / (72.0 * math.sqrt(L * L * L))
    value = acc[...] * scale
    kr, ki = value[0:16], value[16:32]
    cbuf[0, :, 0:32] = kr[:, 0:32] - ki[:, 32:64]
    cbuf[1, :, 0:32] = kr[:, 32:64] + ki[:, 0:32]
    for current in range(NG):
        g = gtab[current]
        for part in range(2):
            ex[current // 8, part, pl.ds(current % 8, 1), :] = cbuf[part, pl.ds(g, 1), :]
    swap = pltpu.make_async_remote_copy(
        src_ref=ex.at[1 - gz],
        dst_ref=rx,
        send_sem=ex_send,
        recv_sem=ex_recv,
        device_id=(ta, 1 - gz),
        device_id_type=MESH,
    )
    swap.start()
    swap.wait()
    for part in range(2):
        out[part, 0] = (ex[gz, part] + rx[part])[:, 0:NP]


def body(propagator, backward, sink_time, source_position, momenta, gamma_table):
    vmem, smem = pltpu.VMEM, pltpu.SMEM
    tile = (1, 1024)
    return pl.pallas_call(
        kernel,
        out_shape=jax.ShapeDtypeStruct((2, 1, 8, NP), F32),
        in_specs=[pl.BlockSpec(memory_space=pl.ANY)] * 2 + [pl.BlockSpec(memory_space=smem)] * 5,
        out_specs=pl.BlockSpec(memory_space=vmem),
        scratch_shapes=[
            vmem((CHUNKS, 2, 12, 12) + tile, F32),
            vmem((CHUNKS, 2, 12, 12) + tile, F32),
            vmem((CHUNKS, 6, 26) + tile, F32),
            vmem((SLOTS, 6, 7) + tile, F32),
            vmem((6, SLOTS // 2 * 13) + tile, F32),
            vmem((OUT_RING, 6, 7) + tile, F32),
            vmem((3, 78) + tile, F32),
            vmem((3, 12) + tile, F32),
            vmem((12, 12) + tile, F32),
            vmem((2, 4, 4) + tile, F32),
            vmem((32, 1024), F32),
            vmem((CHUNKS, 4, 64, 256), jnp.bfloat16),
            vmem((CHUNKS, 4, 64, 256), jnp.bfloat16),
            vmem((3, 32, 128), F32),
            vmem((32, 64), F32),
            vmem((2, 16, 128), F32),
            vmem((2, 2, 8, 128), F32),
            vmem((2, 8, 128), F32),
            pltpu.SemaphoreType.DMA((CHUNKS,)),
            pltpu.SemaphoreType.DMA((CHUNKS,)),
            pltpu.SemaphoreType.DMA((OUT_RING, 6)),
            pltpu.SemaphoreType.DMA((SEM_RING, 6)),
            pltpu.SemaphoreType.DMA,
            pltpu.SemaphoreType.DMA,
        ],
        compiler_params=pltpu.CompilerParams(
            collective_id=0, has_side_effects=True, vmem_limit_bytes=67_000_000
        ),
    )(
        propagator,
        backward,
        jnp.asarray(tree_words()),
        sink_time,
        source_position,
        jnp.transpose(momenta),
        gamma_table,
    )


def solution(mesh):
    in_specs = (
        P(None, None, None, "ta", "gz"),
        P(None, None, None, "ta", "gz"),
        P(),
        P(),
        P(),
        P(),
    )
    out_specs = P(None, "ta", "gz", None)
    return jax.shard_map(body, mesh=mesh, in_specs=in_specs, out_specs=out_specs, check_vma=False)
```

```python
import functools
import itertools
import math

import jax
import jax.numpy as jnp
import numpy as np
from jax import lax
from jax.experimental import pallas as pl
from jax.experimental.pallas import tpu as pltpu
from jax.sharding import PartitionSpec as P

L = 24
NG = 16
NP = 27
CHUNKS = 7
LAG = 6
PACKETS = 4 * CHUNKS
DEPTH = 7
MOST_SLOTS = PACKETS + DEPTH * LAG
LINE = MOST_SLOTS // 2 * 13
OWN = 6 * LINE
OUT_RING = 4
STEPS = ((1, 0, 0), (-1, 0, 0), (0, 1, 0), (0, -1, 0), (0, 0, 1), (0, 0, -1))
TREE_STEPS = (0, 3, 4, 1, 2, 5)
MESH = pl.DeviceIdType.MESH
F32 = jnp.float32


def moved(v, step, sign=1):
    return tuple((a + sign * b) % 4 for a, b in zip(v, step))


def turned(v):
    return tuple((-c) % 4 for c in (v[2], v[0], v[1]))


def turned_step(d):
    return tuple(-c for c in (d[2], d[0], d[1]))


@functools.cache
def tree_words():
    nodes = list(itertools.product(range(4), repeat=3))
    root, child = (0, 0, 0), (1, 0, 0)

    def level(v):
        return sum(min((a - b) % 4, (b - a) % 4) for a, b in zip(v, child))

    def orbit(tail, step):
        while step != (1, 0, 0):
            tail, step = turned(tail), turned_step(step)
        return tail

    taken = orbit(root, (1, 0, 0))
    options = {
        v: [
            (orbit(moved(v, d, -1), d), d)
            for d in STEPS
            if moved(v, d, -1) != root and level(moved(v, d, -1)) < level(v)
        ]
        for v in nodes
        if v not in (root, child)
    }
    match = {}

    def augment(v, seen):
        for key, d in options[v]:
            if key == taken or key in seen:
                continue
            seen.add(key)
            if key not in match or augment(match[key][0], seen):
                match[key] = (v, d)
                return True
        return False

    for v in options:
        assert augment(v, set())
    into = {child: (1, 0, 0)}
    for v, d in match.values():
        into[v] = d
    depth = {root: 0}

    def depth_of(v):
        if v not in depth:
            depth[v] = depth_of(moved(v, into[v], -1)) + 1
        return depth[v]

    edges = [(v, d) for v, d in into.items()]
    depths = {v: depth_of(v) for v in nodes}
    words = np.zeros((3, 64), np.int32)

    def number(v):
        return (v[0] * 4 + v[1]) * 4 + v[2]

    seen_edges = set()
    for k in range(6):
        assert STEPS.index([d for v, d in edges if moved(v, d, -1) == root][0]) == TREE_STEPS[k]
        for v, d in edges:
            n, j = number(v), STEPS.index(d)
            tail = number(moved(v, d, -1))
            assert (tail, j) not in seen_edges
            seen_edges.add((tail, j))
            words[0, n] |= j << (3 * k)
            words[1, tail] |= k << (3 * j)
        for v, n_hops in depths.items():
            assert n_hops <= DEPTH
            words[2, number(v)] |= n_hops << (3 * k)
        edges = [(turned(v), turned_step(d)) for v, d in edges]
        depths = {turned(v): n_hops for v, n_hops in depths.items()}
    return words.reshape(-1)


PAIRS = [(i, j) for i in range(12) for j in range(i, 12)]
PAIR_NUMBER = {p: n for n, p in enumerate(PAIRS)}


def pair_number(i, j):
    return PAIR_NUMBER[(min(i, j), max(i, j))]


def kernel(
    prop, back, sink_in, origin_in, momenta_in, gtab_in, out,
    sv, hv, inbox, stream, outbox, sig, hsum, ssum, macc, kbuf, ph_hi, ph_lo,
    mom, acc, cbuf, ex, rx, words, sink, origin, momenta, gtab,
    s_sem, h_sem, send_sem, recv_sem, ex_send, ex_recv, small_sem,
):
    ta = lax.axis_index("ta")
    gz = lax.axis_index("gz")
    cy, cx, cz = ta // 16, (ta // 4) % 4, ta % 4

    def load(src, dst, sem, c):
        sites = 1024 if c < CHUNKS - 1 else 768
        return pltpu.make_async_copy(
            src.at[:, :, :, :, pl.ds(1024 * c, sites)],
            dst.at[c, :, :, :, :, pl.ds(0, sites)],
            sem.at[c],
        )

    small = [
        pltpu.make_async_copy(src, dst, small_sem.at[i])
        for i, (src, dst) in enumerate(
            ((sink_in, sink), (origin_in, origin), (momenta_in, momenta), (gtab_in, gtab))
        )
    ]
    for copy in small:
        copy.start()
    for c in range(CHUNKS):
        load(prop, sv, s_sem, c).start()
        load(back, hv, h_sem, c).start()

    def neighbour(d):
        x, y, z = STEPS[d]
        return ((cy + y + 4) % 4 * 4 + (cx + x + 4) % 4) * 4 + (cz + z + 4) % 4

    barrier = pltpu.get_barrier_semaphore()
    for d in range(6):
        pl.semaphore_signal(barrier, inc=1, device_id=(neighbour(d), gz), device_id_type=MESH)
    pl.semaphore_signal(barrier, inc=1, device_id=(ta, 1 - gz), device_id_type=MESH)

    for n, word in enumerate(tree_words().tolist()):
        words[n] = jnp.int32(word)
    small[0].wait()
    root = sink[0]
    rel_x = (cx - root // 4 % 4 + 4) % 4
    rel_y = (cy - root // 16 + 4) % 4
    rel_z = (cz - root % 4 + 4) % 4
    rel = (rel_x * 4 + rel_y) * 4 + rel_z
    is_root = rel == 0
    into_word, from_word, depth_word = words[rel], words[64 + rel], words[128 + rel]
    into = [(into_word >> (3 * k)) & 7 for k in range(6)]
    out_of = [(from_word >> (3 * d)) & 7 for d in range(6)]
    depth = [(depth_word >> (3 * k)) & 7 for k in range(6)]

    def source(c, part):
        lo, hi = ((0, 4), (4, 7), (7, 10), (10, 13))[part]
        for k in range(6):
            for n in range(lo, hi):
                i, j = PAIRS[6 * n + k]
                re = im = None
                for m in range(12):
                    a, b = sv[c, 0, i, m], sv[c, 1, i, m]
                    if i == j:
                        r, q = a * a - b * b, a * b
                        q = q + q
                    else:
                        e, f = sv[c, 0, j, m], sv[c, 1, j, m]
                        r, q = a * e - b * f, a * f + b * e
                    re = r if re is None else re + r
                    im = q if im is None else im + q
                at = OWN + 26 * CHUNKS * k + 26 * c + 2 * n
                stream[at] = re
                stream[at + 1] = im

    def phases(chunk, pairs):
        lane = lax.broadcasted_iota(jnp.int32, (32, 128), 1).astype(F32)
        ox, oy, oz = (origin[i].astype(F32) for i in range(3))
        px, py, pz = mom[0], mom[1], mom[2]
        start = (gz * 6912 + chunk * 1024).astype(F32)
        for pair in pairs:
            for half in range(2):
                site = lane[0:8] + (start + (256.0 * pair + 128.0 * half))
                z = jnp.floor((site + 0.5) * (1.0 / 576.0))
                rest = site - z * 576.0
                x = jnp.floor((rest + 0.5) * (1.0 / 24.0))
                y = rest - x * 24.0
                x, y, z = (jnp.concatenate([v] * 4, axis=0) for v in (x - ox, y - oy, z - oz))
                wave = px * x + py * y + pz * z
                wave = wave - 24.0 * jnp.floor(wave * (1.0 / 24.0) + 0.5)
                angle = wave * (math.pi / L)
                square = angle * angle
                s = c = None
                for n in range(13, 0, -2):
                    term = (-1.0) ** (n // 2) / math.factorial(n)
                    s = term if s is None else s * square + term
                for n in range(12, -1, -2):
                    term = (-1.0) ** (n // 2) / math.factorial(n)
                    c = term if c is None else c * square + term
                s = s * angle
                twice = s + s
                for row, value in ((0, 1.0 - twice * s), (32, -(twice * c))):
                    hi = value.astype(jnp.bfloat16)
                    at = (chunk + 1, pair, pl.ds(row, 32), pl.ds(128 * half, 128))
                    ph_hi[at] = hi
                    ph_lo[at] = (value - hi.astype(F32)).astype(jnp.bfloat16)

    def sums(c, src, dst):
        for i in range(12):
            for m in range(12):
                dst[c, i, m] = src[c, 0, i, m] + src[c, 1, i, m]

    def unpack(c, block, base):
        first, last = ((0, 6), (6, 10), (10, 13))[block]
        for n in range(first, last):
            for k in range(6):
                at = base[k] + c * 26 + 2 * n
                sig[6 * n + k] = stream[at] + stream[at + 1]

    def plus(x, y):
        return y if x is None else x + y

    def contract(c, block, base):
        columns = range(3 * block, 3 * block + 3)

        def one(al):
            part = {(a, m): [None] * 3 for a in range(3) for m in columns}
            for k in range(12):
                rows = [3 * al + a for a in range(3)]
                left = [(hv[c, 0, r, k], hv[c, 1, r, k], hsum[c, r, k]) for r in rows]
                for m in columns:
                    n = pair_number(k, m)
                    at = base[n % 6] + c * 26 + n // 6 * 2
                    right = (stream[at], stream[at + 1], sig[n])
                    for a in range(3):
                        for t in range(3):
                            part[a, m][t] = plus(part[a, m][t], left[a][t] * right[t])
            total = [[None] * 3 for _ in range(4)]
            for a in range(3):
                for m in columns:
                    p1, p2, p3 = part[a, m]
                    br, bi = p1 - p2, p3 - (p1 + p2)
                    bound = (br, bi, br - bi)
                    for be in range(4):
                        row = 3 * be + a
                        forward = (sv[c, 0, row, m], sv[c, 1, row, m], ssum[c, row, m])
                        for t in range(3):
                            total[be][t] = plus(total[be][t], forward[t] * bound[t])
            for be in range(4):
                for t in range(3):
                    value = total[be][t]
                    macc[t, be, al] = value if block == 0 else macc[t, be, al] + value

        @pl.loop(0, 2)
        def _(half):
            one(2 * half)
            one(2 * half + 1)

    def add(p, q):
        return (p[0] + q[0], p[1] + q[1])

    def sub(p, q):
        return (p[0] - q[0], p[1] - q[1])

    def pauli(m):
        d = sub(m[0][1], m[1][0])
        return [add(m[0][0], m[1][1]), add(m[1][0], m[0][1]), (-d[1], d[0]), sub(m[0][0], m[1][1])]

    def entry(be, al):
        m0, m1, m2 = macc[0, be, al], macc[1, be, al], macc[2, be, al]
        return (m0 + m1, m2 - (m0 - m1))

    def project(c):
        inner = [
            [
                pauli(
                    [
                        [
                            entry(2 * b1 + b0, 2 * a1 + a0)
                            for a0 in range(2)
                        ]
                        for b0 in range(2)
                    ]
                )
                for a1 in range(2)
            ]
            for b1 in range(2)
        ]
        site = lax.broadcasted_iota(jnp.int32, (1, 1024), 1)
        valid = (site < 768) | (c < CHUNKS - 1)
        for low in range(4):
            outer = pauli([[inner[b1][a1][low] for a1 in range(2)] for b1 in range(2)])
            for high in range(4):
                n = 4 * high + low
                for part in range(2):
                    kbuf[pl.ds(16 * part + n, 1), :] = jnp.where(valid, outer[high][part], 0.0)
        result = acc[...]
        dims = (((1,), (1,)), ((), ()))
        for pair in range(4):
            left = kbuf[:, pl.ds(256 * pair, 256)]
            hi = left.astype(jnp.bfloat16)
            lo = (left - hi.astype(F32)).astype(jnp.bfloat16)
            for x, y in ((hi, ph_hi), (lo, ph_hi), (hi, ph_lo)):
                result = result + lax.dot_general(
                    x, y[c + 1, pair], dims, preferred_element_type=F32
                )
        acc[...] = result

    acc[...] = jnp.zeros_like(acc)
    macc[...] = jnp.zeros_like(macc)
    ph_hi[0] = jnp.zeros((4, 64, 256), jnp.bfloat16)
    ph_lo[0] = jnp.zeros((4, 64, 256), jnp.bfloat16)
    for copy in small[1:]:
        copy.wait()
    mom[...] = jnp.zeros_like(mom)
    for p in range(NP):
        for i in range(3):
            mom[i, pl.ds(p, 1), :] = jnp.full((1, 128), momenta[i, p], jnp.int32).astype(F32)
    load(prop, sv, s_sem, 0).wait()
    source(0, 0)
    pl.semaphore_wait(barrier, 7)

    lag = LAG - 2 * gz
    shift = 13 * LAG // 2 - 13 * gz
    base = [
        jnp.where(is_root, OWN + 26 * CHUNKS * k, LINE * into[k] + depth[k] * shift)
        for k in range(6)
    ]
    line = [sum(jnp.where(out_of[d] == k, LINE * into[k], 0) for k in range(6)) for d in range(6)]
    own_line = [
        jnp.where(is_root, OWN + 26 * CHUNKS * TREE_STEPS.index(d), line[d]) for d in range(6)
    ]

    def message(s, ring, tiles, d=None):
        links = pl.ds(0, 6) if d is None else d
        return pltpu.make_async_remote_copy(
            src_ref=outbox.at[ring, links, pl.ds(0, tiles)],
            dst_ref=inbox.at[s + lag, links, pl.ds(0, tiles)],
            send_sem=send_sem.at[ring],
            recv_sem=recv_sem.at[s + lag],
            device_id=(neighbour(d or 0), gz),
            device_id_type=MESH,
        )

    def arrive(s, ring, tiles, flat):
        message(s - lag, ring, tiles).wait_recv()
        for d in range(6):
            for i in range(tiles):
                stream[LINE * d + flat + i] = inbox[s, d, i]

    def send(s, ring, tiles, flat, first_slots=False):
        if first_slots:
            pl.when(s >= OUT_RING)(message(s - OUT_RING, ring, tiles).wait_send)
        else:
            message(s - OUT_RING, ring, tiles).wait_send()
        at = own_line if first_slots else line
        for d in range(6):
            for i in range(tiles):
                outbox[ring, d, i] = stream[at[d] + flat + i]
        for d in range(6):
            message(s, ring, tiles, d).start()

    @pl.loop(0, CHUNKS)
    def _(g):
        for u in range(4):
            s = 4 * g + u
            slot = (s, u, 7 - u % 2, 26 * g + 13 * (u // 2) + 7 * (u % 2))
            pl.when(s >= lag)(functools.partial(arrive, *slot))
            send(*slot, first_slots=True)
            if u < 3:
                source(g, u + 1)
            else:
                @pl.when(g < CHUNKS - 1)
                def _():
                    for c in range(1, CHUNKS):
                        @pl.when(g + 1 == c)
                        def _(c=c):
                            load(prop, sv, s_sem, c).wait()

                    source(g + 1, 0)
            if u == 2:
                for c in range(CHUNKS):
                    @pl.when(g == c)
                    def _(c=c):
                        load(back, hv, h_sem, c).wait()

            if u % 2 == 0:
                sums(g, *((sv, ssum), (hv, hsum))[u // 2])
            else:
                phases(g, (u - 1, u))

    slot = (PACKETS, 0, 7, PACKETS // 2 * 13)
    arrive(*slot)
    send(*slot)

    @pl.loop(0, DEPTH - DEPTH * gz)
    def _(p):
        for odd in (1, 0):
            s = PACKETS + 2 * p + 2 - odd
            slot = (s, s % OUT_RING, 7 - odd, (PACKETS // 2 + p + 1 - odd) * 13 + 7 * odd)
            arrive(*slot)
            send(*slot)

    @pl.loop(0, CHUNKS)
    def _(c):
        for block in range(4):
            s = DEPTH * lag + 1 + 4 * c + block
            u = (3 + block) % 4
            ring = u + 2 * gz if u < 2 else u - 2 * gz
            odd = u % 2
            pair = DEPTH * LAG // 2 - DEPTH * gz + 2 * c + (1 + block) // 2
            slot = (s, ring, 7 - odd, 13 * pair + 7 * odd)
            pl.when(4 * c + block < PACKETS - 1)(functools.partial(arrive, *slot))
            pl.when(4 * c + block < PACKETS - 1 - lag)(functools.partial(send, *slot))
            if block == 0:
                project(c - 1)
            if block < 3:
                unpack(c, block, base)
            contract(c, block, base)

    project(CHUNKS - 1)
    for ring in range(4):
        s = PACKETS + (DEPTH - 1) * lag - 4 + ring
        message(s, ring, 7 - ring % 2).wait_send()

    scale = 0.125 / (72.0 * math.sqrt(L * L * L))
    value = acc[...] * scale
    kr, ki = value[0:16], value[16:32]
    cbuf[0, :, 0:32] = kr[:, 0:32] - ki[:, 32:64]
    cbuf[1, :, 0:32] = kr[:, 32:64] + ki[:, 0:32]
    for current in range(NG):
        g = gtab[current]
        for part in range(2):
            ex[current // 8, part, pl.ds(current % 8, 1), :] = cbuf[part, pl.ds(g, 1), :]
    swap = pltpu.make_async_remote_copy(
        src_ref=ex.at[1 - gz],
        dst_ref=rx,
        send_sem=ex_send,
        recv_sem=ex_recv,
        device_id=(ta, 1 - gz),
        device_id_type=MESH,
    )
    swap.start()
    swap.wait()
    for part in range(2):
        out[part, 0] = (ex[gz, part] + rx[part])[:, 0:NP]


def body(propagator, backward, sink_time, source_position, momenta, gamma_table):
    vmem, smem = pltpu.VMEM, pltpu.SMEM
    tile = (1, 1024)
    return pl.pallas_call(
        kernel,
        out_shape=jax.ShapeDtypeStruct((2, 1, 8, NP), F32),
        in_specs=[pl.BlockSpec(memory_space=pl.ANY)] * 6,
        out_specs=pl.BlockSpec(memory_space=vmem),
        scratch_shapes=[
            vmem((CHUNKS, 2, 12, 12) + tile, F32),
            vmem((CHUNKS, 2, 12, 12) + tile, F32),
            vmem((MOST_SLOTS, 6, 7) + tile, F32),
            vmem((OWN + 6 * 26 * CHUNKS,) + tile, F32),
            vmem((OUT_RING, 6, 7) + tile, F32),
            vmem((78,) + tile, F32),
            vmem((CHUNKS, 12, 12) + tile, F32),
            vmem((CHUNKS, 12, 12) + tile, F32),
            vmem((3, 4, 4) + tile, F32),
            vmem((32, 1024), F32),
            vmem((CHUNKS + 1, 4, 64, 256), jnp.bfloat16),
            vmem((CHUNKS + 1, 4, 64, 256), jnp.bfloat16),
            vmem((3, 32, 128), F32),
            vmem((32, 64), F32),
            vmem((2, 16, 128), F32),
            vmem((2, 2, 8, 128), F32),
            vmem((2, 8, 128), F32),
            smem((192,), jnp.int32),
            smem((1,), jnp.int32),
            smem((3,), jnp.int32),
            smem((3, NP), jnp.int32),
            smem((NG,), jnp.int32),
            pltpu.SemaphoreType.DMA((CHUNKS,)),
            pltpu.SemaphoreType.DMA((CHUNKS,)),
            pltpu.SemaphoreType.DMA((OUT_RING,)),
            pltpu.SemaphoreType.DMA((MOST_SLOTS,)),
            pltpu.SemaphoreType.DMA,
            pltpu.SemaphoreType.DMA,
            pltpu.SemaphoreType.DMA((4,)),
        ],
        compiler_params=pltpu.CompilerParams(
            collective_id=0, has_side_effects=True, vmem_limit_bytes=67_000_000
        ),
    )(
        propagator,
        backward,
        sink_time,
        source_position,
        jnp.transpose(momenta),
        gamma_table,
    )


def solution(mesh):
    in_specs = (
        P(None, None, None, "ta", "gz"),
        P(None, None, None, "ta", "gz"),
        P(),
        P(),
        P(),
        P(),
    )
    out_specs = P(None, "ta", "gz", None)
    return jax.shard_map(body, mesh=mesh, in_specs=in_specs, out_specs=out_specs, check_vma=False)
```

```python
import functools
import itertools
import math

import jax
import jax.numpy as jnp
import numpy as np
from jax import lax
from jax.experimental import pallas as pl
from jax.experimental.pallas import tpu as pltpu
from jax.sharding import PartitionSpec as P

L = 24
NG = 16
NP = 27
CHUNKS = 7
LAG = 6
PACKETS = 4 * CHUNKS
DEPTH = 7
MOST_SLOTS = PACKETS + DEPTH * LAG
LINE = MOST_SLOTS // 2 * 13
OWN = 6 * LINE
OUT_RING = 4
STEPS = ((1, 0, 0), (-1, 0, 0), (0, 1, 0), (0, -1, 0), (0, 0, 1), (0, 0, -1))
TREE_STEPS = (0, 3, 4, 1, 2, 5)
MESH = pl.DeviceIdType.MESH
F32 = jnp.float32


def moved(v, step, sign=1):
    return tuple((a + sign * b) % 4 for a, b in zip(v, step))


def turned(v):
    return tuple((-c) % 4 for c in (v[2], v[0], v[1]))


def turned_step(d):
    return tuple(-c for c in (d[2], d[0], d[1]))


@functools.cache
def tree_words():
    nodes = list(itertools.product(range(4), repeat=3))
    root, child = (0, 0, 0), (1, 0, 0)

    def level(v):
        return sum(min((a - b) % 4, (b - a) % 4) for a, b in zip(v, child))

    def orbit(tail, step):
        while step != (1, 0, 0):
            tail, step = turned(tail), turned_step(step)
        return tail

    taken = orbit(root, (1, 0, 0))
    options = {
        v: [
            (orbit(moved(v, d, -1), d), d)
            for d in STEPS
            if moved(v, d, -1) != root and level(moved(v, d, -1)) < level(v)
        ]
        for v in nodes
        if v not in (root, child)
    }
    match = {}

    def augment(v, seen):
        for key, d in options[v]:
            if key == taken or key in seen:
                continue
            seen.add(key)
            if key not in match or augment(match[key][0], seen):
                match[key] = (v, d)
                return True
        return False

    for v in options:
        assert augment(v, set())
    into = {child: (1, 0, 0)}
    for v, d in match.values():
        into[v] = d
    depth = {root: 0}

    def depth_of(v):
        if v not in depth:
            depth[v] = depth_of(moved(v, into[v], -1)) + 1
        return depth[v]

    edges = [(v, d) for v, d in into.items()]
    depths = {v: depth_of(v) for v in nodes}
    words = np.zeros((3, 64), np.int32)

    def number(v):
        return (v[0] * 4 + v[1]) * 4 + v[2]

    seen_edges = set()
    for k in range(6):
        assert STEPS.index([d for v, d in edges if moved(v, d, -1) == root][0]) == TREE_STEPS[k]
        for v, d in edges:
            n, j = number(v), STEPS.index(d)
            tail = number(moved(v, d, -1))
            assert (tail, j) not in seen_edges
            seen_edges.add((tail, j))
            words[0, n] |= j << (3 * k)
            words[1, tail] |= k << (3 * j)
        for v, n_hops in depths.items():
            assert n_hops <= DEPTH
            words[2, number(v)] |= n_hops << (3 * k)
        edges = [(turned(v), turned_step(d)) for v, d in edges]
        depths = {turned(v): n_hops for v, n_hops in depths.items()}
    return words.reshape(-1)


PAIRS = [(i, j) for i in range(12) for j in range(i, 12)]
PAIR_NUMBER = {p: n for n, p in enumerate(PAIRS)}


def pair_number(i, j):
    return PAIR_NUMBER[(min(i, j), max(i, j))]


def kernel(
    prop, back, sink_in, origin_in, momenta_in, gtab_in, out,
    sv, hv, inbox, stream, outbox, sig, hsum, ssum, macc, kbuf, ph_hi, ph_lo,
    mom, acc, cbuf, rx, words, sink, origin, momenta, gtab,
    s_sem, h_sem, send_sem, recv_sem, ex_send, ex_recv, small_sem,
):
    ta = lax.axis_index("ta")
    gz = lax.axis_index("gz")
    cy, cx, cz = ta // 16, (ta // 4) % 4, ta % 4

    def load(src, dst, sem, c):
        sites = 1024 if c < CHUNKS - 1 else 768
        return pltpu.make_async_copy(
            src.at[:, :, :, :, pl.ds(1024 * c, sites)],
            dst.at[c, :, :, :, :, pl.ds(0, sites)],
            sem.at[c],
        )

    small = [
        pltpu.make_async_copy(src, dst, small_sem.at[i])
        for i, (src, dst) in enumerate(
            ((sink_in, sink), (origin_in, origin), (momenta_in, momenta), (gtab_in, gtab))
        )
    ]
    for copy in small:
        copy.start()
    for c in range(CHUNKS):
        load(prop, sv, s_sem, c).start()
        load(back, hv, h_sem, c).start()

    def neighbour(d):
        x, y, z = STEPS[d]
        return ((cy + y + 4) % 4 * 4 + (cx + x + 4) % 4) * 4 + (cz + z + 4) % 4

    barrier = pltpu.get_barrier_semaphore()
    for d in range(6):
        pl.semaphore_signal(barrier, inc=1, device_id=(neighbour(d), gz), device_id_type=MESH)
    pl.semaphore_signal(barrier, inc=1, device_id=(ta, 1 - gz), device_id_type=MESH)

    for n, word in enumerate(tree_words().tolist()):
        words[n] = jnp.int32(word)
    small[0].wait()
    root = sink[0]
    rel_x = (cx - root // 4 % 4 + 4) % 4
    rel_y = (cy - root // 16 + 4) % 4
    rel_z = (cz - root % 4 + 4) % 4
    rel = (rel_x * 4 + rel_y) * 4 + rel_z
    is_root = rel == 0
    into_word, from_word, depth_word = words[rel], words[64 + rel], words[128 + rel]
    into = [(into_word >> (3 * k)) & 7 for k in range(6)]
    out_of = [(from_word >> (3 * d)) & 7 for d in range(6)]
    depth = [(depth_word >> (3 * k)) & 7 for k in range(6)]

    def source(c, part):
        lo, hi = ((0, 4), (4, 7), (7, 10), (10, 13))[part]
        for k in range(6):
            for n in range(lo, hi):
                i, j = PAIRS[6 * n + k]
                re = im = None
                for m in range(12):
                    a, b = sv[c, 0, i, m], sv[c, 1, i, m]
                    if i == j:
                        r, q = a * a - b * b, a * b
                        q = q + q
                    else:
                        e, f = sv[c, 0, j, m], sv[c, 1, j, m]
                        r, q = a * e - b * f, a * f + b * e
                    re = r if re is None else re + r
                    im = q if im is None else im + q
                at = OWN + 26 * CHUNKS * k + 26 * c + 2 * n
                stream[at] = re
                stream[at + 1] = im

    def phases(chunk, pairs):
        lane = lax.broadcasted_iota(jnp.int32, (32, 128), 1).astype(F32)
        ox, oy, oz = (origin[i].astype(F32) for i in range(3))
        px, py, pz = mom[0], mom[1], mom[2]
        start = (gz * 6912 + chunk * 1024).astype(F32)
        for pair in pairs:
            for half in range(2):
                site = lane[0:8] + (start + (256.0 * pair + 128.0 * half))
                z = jnp.floor((site + 0.5) * (1.0 / 576.0))
                rest = site - z * 576.0
                x = jnp.floor((rest + 0.5) * (1.0 / 24.0))
                y = rest - x * 24.0
                x, y, z = (jnp.concatenate([v] * 4, axis=0) for v in (x - ox, y - oy, z - oz))
                wave = px * x + py * y + pz * z
                wave = wave - 24.0 * jnp.floor(wave * (1.0 / 24.0) + 0.5)
                angle = wave * (math.pi / L)
                square = angle * angle
                s = c = None
                for n in range(13, 0, -2):
                    term = (-1.0) ** (n // 2) / math.factorial(n)
                    s = term if s is None else s * square + term
                for n in range(12, -1, -2):
                    term = (-1.0) ** (n // 2) / math.factorial(n)
                    c = term if c is None else c * square + term
                s = s * angle
                twice = s + s
                for row, value in ((0, 1.0 - twice * s), (32, -(twice * c))):
                    hi = value.astype(jnp.bfloat16)
                    at = (chunk + 1, pair, pl.ds(row, 32), pl.ds(128 * half, 128))
                    ph_hi[at] = hi
                    ph_lo[at] = (value - hi.astype(F32)).astype(jnp.bfloat16)

    def sums(c, src, dst):
        for i in range(12):
            for m in range(12):
                dst[c, i, m] = src[c, 0, i, m] + src[c, 1, i, m]

    def unpack(c, block, base):
        first, last = ((0, 6), (6, 10), (10, 13))[block]
        for n in range(first, last):
            for k in range(6):
                at = base[k] + c * 26 + 2 * n
                sig[6 * n + k] = stream[at] + stream[at + 1]

    def plus(x, y):
        return y if x is None else x + y

    def contract(c, block, base):
        columns = range(3 * block, 3 * block + 3)

        def one(al):
            part = {(a, m): [None] * 3 for a in range(3) for m in columns}
            for k in range(12):
                rows = [3 * al + a for a in range(3)]
                left = [(hv[c, 0, r, k], hv[c, 1, r, k], hsum[c, r, k]) for r in rows]
                for m in columns:
                    n = pair_number(k, m)
                    at = base[n % 6] + c * 26 + n // 6 * 2
                    right = (stream[at], stream[at + 1], sig[n])
                    for a in range(3):
                        for t in range(3):
                            part[a, m][t] = plus(part[a, m][t], left[a][t] * right[t])
            total = [[None] * 3 for _ in range(4)]
            for a in range(3):
                for m in columns:
                    p1, p2, p3 = part[a, m]
                    br, bi = p1 - p2, p3 - (p1 + p2)
                    bound = (br, bi, br - bi)
                    for be in range(4):
                        row = 3 * be + a
                        forward = (sv[c, 0, row, m], sv[c, 1, row, m], ssum[c, row, m])
                        for t in range(3):
                            total[be][t] = plus(total[be][t], forward[t] * bound[t])
            for be in range(4):
                for t in range(3):
                    value = total[be][t]
                    macc[t, be, al] = value if block == 0 else macc[t, be, al] + value

        for al in range(4):
            one(al)

    def add(p, q):
        return (p[0] + q[0], p[1] + q[1])

    def sub(p, q):
        return (p[0] - q[0], p[1] - q[1])

    def pauli(m):
        d = sub(m[0][1], m[1][0])
        return [add(m[0][0], m[1][1]), add(m[1][0], m[0][1]), (-d[1], d[0]), sub(m[0][0], m[1][1])]

    def entry(be, al):
        m0, m1, m2 = macc[0, be, al], macc[1, be, al], macc[2, be, al]
        return (m0 + m1, m2 - (m0 - m1))

    def project(c):
        inner = [
            [
                pauli(
                    [
                        [
                            entry(2 * b1 + b0, 2 * a1 + a0)
                            for a0 in range(2)
                        ]
                        for b0 in range(2)
                    ]
                )
                for a1 in range(2)
            ]
            for b1 in range(2)
        ]
        site = lax.broadcasted_iota(jnp.int32, (1, 1024), 1)
        valid = (site < 768) | (c < CHUNKS - 1)
        for low in range(4):
            outer = pauli([[inner[b1][a1][low] for a1 in range(2)] for b1 in range(2)])
            for high in range(4):
                n = 4 * high + low
                for part in range(2):
                    kbuf[pl.ds(16 * part + n, 1), :] = jnp.where(valid, outer[high][part], 0.0)
        result = acc[...]
        dims = (((1,), (1,)), ((), ()))
        for pair in range(4):
            left = kbuf[:, pl.ds(256 * pair, 256)]
            hi = left.astype(jnp.bfloat16)
            lo = (left - hi.astype(F32)).astype(jnp.bfloat16)
            both = jnp.concatenate([hi, lo], axis=0)
            main = lax.dot_general(both, ph_hi[c + 1, pair], dims, preferred_element_type=F32)
            rest = lax.dot_general(hi, ph_lo[c + 1, pair], dims, preferred_element_type=F32)
            result = result + (main[0:32] + main[32:64] + rest)
        acc[...] = result

    acc[...] = jnp.zeros_like(acc)
    macc[...] = jnp.zeros_like(macc)
    ph_hi[0] = jnp.zeros((4, 64, 256), jnp.bfloat16)
    ph_lo[0] = jnp.zeros((4, 64, 256), jnp.bfloat16)
    for copy in small[1:]:
        copy.wait()
    mom[...] = jnp.zeros_like(mom)
    for p in range(NP):
        for i in range(3):
            mom[i, pl.ds(p, 1), :] = jnp.full((1, 128), momenta[i, p], jnp.int32).astype(F32)
    load(prop, sv, s_sem, 0).wait()
    source(0, 0)
    pl.semaphore_wait(barrier, 7)

    lag = LAG - 2 * gz
    shift = 13 * LAG // 2 - 13 * gz
    base = [
        jnp.where(is_root, OWN + 26 * CHUNKS * k, LINE * into[k] + depth[k] * shift)
        for k in range(6)
    ]
    line = [sum(jnp.where(out_of[d] == k, LINE * into[k], 0) for k in range(6)) for d in range(6)]
    own_line = [
        jnp.where(is_root, OWN + 26 * CHUNKS * TREE_STEPS.index(d), line[d]) for d in range(6)
    ]

    def message(s, ring, tiles, d=None):
        links = pl.ds(0, 6) if d is None else d
        return pltpu.make_async_remote_copy(
            src_ref=outbox.at[ring, links, pl.ds(0, tiles)],
            dst_ref=inbox.at[s + lag, links, pl.ds(0, tiles)],
            send_sem=send_sem.at[ring],
            recv_sem=recv_sem.at[s + lag],
            device_id=(neighbour(d or 0), gz),
            device_id_type=MESH,
        )

    def arrive(s, ring, tiles, flat):
        message(s - lag, ring, tiles).wait_recv()
        for d in range(6):
            for i in range(tiles):
                stream[LINE * d + flat + i] = inbox[s, d, i]

    def send(s, ring, tiles, flat, first_slots=False):
        if first_slots:
            pl.when(s >= OUT_RING)(message(s - OUT_RING, ring, tiles).wait_send)
        else:
            message(s - OUT_RING, ring, tiles).wait_send()
        at = own_line if first_slots else line
        for d in range(6):
            for i in range(tiles):
                outbox[ring, d, i] = stream[at[d] + flat + i]
        for d in range(6):
            message(s, ring, tiles, d).start()

    @pl.loop(0, CHUNKS)
    def _(g):
        for u in range(4):
            s = 4 * g + u
            slot = (s, u, 7 - u % 2, 26 * g + 13 * (u // 2) + 7 * (u % 2))
            pl.when(s >= lag)(functools.partial(arrive, *slot))
            send(*slot, first_slots=True)
            if u < 3:
                source(g, u + 1)
            else:
                @pl.when(g < CHUNKS - 1)
                def _():
                    for c in range(1, CHUNKS):
                        @pl.when(g + 1 == c)
                        def _(c=c):
                            load(prop, sv, s_sem, c).wait()

                    source(g + 1, 0)
            if u == 2:
                for c in range(CHUNKS):
                    @pl.when(g == c)
                    def _(c=c):
                        load(back, hv, h_sem, c).wait()

            if u % 2 == 0:
                sums(g, *((sv, ssum), (hv, hsum))[u // 2])
            else:
                phases(g, (u - 1, u))

    slot = (PACKETS, 0, 7, PACKETS // 2 * 13)
    arrive(*slot)
    send(*slot)

    @pl.loop(0, DEPTH - DEPTH * gz)
    def _(p):
        for odd in (1, 0):
            s = PACKETS + 2 * p + 2 - odd
            slot = (s, s % OUT_RING, 7 - odd, (PACKETS // 2 + p + 1 - odd) * 13 + 7 * odd)
            arrive(*slot)
            send(*slot)

    @pl.loop(0, CHUNKS)
    def _(c):
        for block in range(4):
            s = DEPTH * lag + 1 + 4 * c + block
            u = (3 + block) % 4
            ring = u + 2 * gz if u < 2 else u - 2 * gz
            odd = u % 2
            pair = DEPTH * LAG // 2 - DEPTH * gz + 2 * c + (1 + block) // 2
            slot = (s, ring, 7 - odd, 13 * pair + 7 * odd)
            pl.when(4 * c + block < PACKETS - 1)(functools.partial(arrive, *slot))
            pl.when(4 * c + block < PACKETS - 1 - lag)(functools.partial(send, *slot))
            if block == 0:
                project(c - 1)
            if block < 3:
                unpack(c, block, base)
            contract(c, block, base)

    project(CHUNKS - 1)
    for ring in range(4):
        s = PACKETS + (DEPTH - 1) * lag - 4 + ring
        message(s, ring, 7 - ring % 2).wait_send()

    swap = pltpu.make_async_remote_copy(
        src_ref=acc,
        dst_ref=rx,
        send_sem=ex_send,
        recv_sem=ex_recv,
        device_id=(ta, 1 - gz),
        device_id_type=MESH,
    )
    swap.start()
    swap.wait()
    scale = 0.125 / (72.0 * math.sqrt(L * L * L))
    value = (acc[...] + rx[...]) * scale
    kr, ki = value[0:16], value[16:32]
    cbuf[0, :, 0:32] = kr[:, 0:32] - ki[:, 32:64]
    cbuf[1, :, 0:32] = kr[:, 32:64] + ki[:, 0:32]
    for row in range(NG // 2):
        g = gtab[NG // 2 * gz + row]
        for part in range(2):
            out[part, 0, pl.ds(row, 1), :] = cbuf[part, pl.ds(g, 1), 0:NP]


def body(propagator, backward, sink_time, source_position, momenta, gamma_table):
    vmem, smem = pltpu.VMEM, pltpu.SMEM
    tile = (1, 1024)
    return pl.pallas_call(
        kernel,
        out_shape=jax.ShapeDtypeStruct((2, 1, 8, NP), F32),
        in_specs=[pl.BlockSpec(memory_space=pl.ANY)] * 6,
        out_specs=pl.BlockSpec(memory_space=vmem),
        scratch_shapes=[
            vmem((CHUNKS, 2, 12, 12) + tile, F32),
            vmem((CHUNKS, 2, 12, 12) + tile, F32),
            vmem((MOST_SLOTS, 6, 7) + tile, F32),
            vmem((OWN + 6 * 26 * CHUNKS,) + tile, F32),
            vmem((OUT_RING, 6, 7) + tile, F32),
            vmem((78,) + tile, F32),
            vmem((CHUNKS, 12, 12) + tile, F32),
            vmem((CHUNKS, 12, 12) + tile, F32),
            vmem((3, 4, 4) + tile, F32),
            vmem((32, 1024), F32),
            vmem((CHUNKS + 1, 4, 64, 256), jnp.bfloat16),
            vmem((CHUNKS + 1, 4, 64, 256), jnp.bfloat16),
            vmem((3, 32, 128), F32),
            vmem((32, 64), F32),
            vmem((2, 16, 128), F32),
            vmem((32, 64), F32),
            smem((192,), jnp.int32),
            smem((1,), jnp.int32),
            smem((3,), jnp.int32),
            smem((3, NP), jnp.int32),
            smem((NG,), jnp.int32),
            pltpu.SemaphoreType.DMA((CHUNKS,)),
            pltpu.SemaphoreType.DMA((CHUNKS,)),
            pltpu.SemaphoreType.DMA((OUT_RING,)),
            pltpu.SemaphoreType.DMA((MOST_SLOTS,)),
            pltpu.SemaphoreType.DMA,
            pltpu.SemaphoreType.DMA,
            pltpu.SemaphoreType.DMA((4,)),
        ],
        compiler_params=pltpu.CompilerParams(
            collective_id=0, has_side_effects=True, vmem_limit_bytes=67_000_000
        ),
    )(
        propagator,
        backward,
        sink_time,
        source_position,
        jnp.transpose(momenta),
        gamma_table,
    )


def solution(mesh):
    in_specs = (
        P(None, None, None, "ta", "gz"),
        P(None, None, None, "ta", "gz"),
        P(),
        P(),
        P(),
        P(),
    )
    out_specs = P(None, "ta", "gz", None)
    return jax.shard_map(body, mesh=mesh, in_specs=in_specs, out_specs=out_specs, check_vma=False)
```

```python
import functools
import itertools
import math

import jax
import jax.numpy as jnp
import numpy as np
from jax import lax
from jax.experimental import pallas as pl
from jax.experimental.pallas import tpu as pltpu
from jax.sharding import PartitionSpec as P

L = 24
NG = 16
NP = 27
CHUNKS = 7
LAG = 6
PACKETS = 4 * CHUNKS
DEPTH = 7
MOST_SLOTS = PACKETS + DEPTH * LAG
LINE = MOST_SLOTS // 2 * 13
OWN = 6 * LINE
OUT_RING = 4
STEPS = ((1, 0, 0), (-1, 0, 0), (0, 1, 0), (0, -1, 0), (0, 0, 1), (0, 0, -1))
TREE_STEPS = (0, 3, 4, 1, 2, 5)
MESH = pl.DeviceIdType.MESH
F32 = jnp.float32


def moved(v, step, sign=1):
    return tuple((a + sign * b) % 4 for a, b in zip(v, step))


def turned(v):
    return tuple((-c) % 4 for c in (v[2], v[0], v[1]))


def turned_step(d):
    return tuple(-c for c in (d[2], d[0], d[1]))


@functools.cache
def tree_words():
    nodes = list(itertools.product(range(4), repeat=3))
    root, child = (0, 0, 0), (1, 0, 0)

    def level(v):
        return sum(min((a - b) % 4, (b - a) % 4) for a, b in zip(v, child))

    def orbit(tail, step):
        while step != (1, 0, 0):
            tail, step = turned(tail), turned_step(step)
        return tail

    taken = orbit(root, (1, 0, 0))
    options = {
        v: [
            (orbit(moved(v, d, -1), d), d)
            for d in STEPS
            if moved(v, d, -1) != root and level(moved(v, d, -1)) < level(v)
        ]
        for v in nodes
        if v not in (root, child)
    }
    match = {}

    def augment(v, seen):
        for key, d in options[v]:
            if key == taken or key in seen:
                continue
            seen.add(key)
            if key not in match or augment(match[key][0], seen):
                match[key] = (v, d)
                return True
        return False

    for v in options:
        assert augment(v, set())
    into = {child: (1, 0, 0)}
    for v, d in match.values():
        into[v] = d
    depth = {root: 0}

    def depth_of(v):
        if v not in depth:
            depth[v] = depth_of(moved(v, into[v], -1)) + 1
        return depth[v]

    edges = [(v, d) for v, d in into.items()]
    depths = {v: depth_of(v) for v in nodes}
    words = np.zeros((3, 64), np.int32)

    def number(v):
        return (v[0] * 4 + v[1]) * 4 + v[2]

    seen_edges = set()
    for k in range(6):
        assert STEPS.index([d for v, d in edges if moved(v, d, -1) == root][0]) == TREE_STEPS[k]
        for v, d in edges:
            n, j = number(v), STEPS.index(d)
            tail = number(moved(v, d, -1))
            assert (tail, j) not in seen_edges
            seen_edges.add((tail, j))
            words[0, n] |= j << (3 * k)
            words[1, tail] |= k << (3 * j)
        for v, n_hops in depths.items():
            assert n_hops <= DEPTH
            words[2, number(v)] |= n_hops << (3 * k)
        edges = [(turned(v), turned_step(d)) for v, d in edges]
        depths = {turned(v): n_hops for v, n_hops in depths.items()}
    return words.reshape(-1)


PAIRS = [(i, j) for i in range(12) for j in range(i, 12)]
PAIR_NUMBER = {p: n for n, p in enumerate(PAIRS)}


def pair_number(i, j):
    return PAIR_NUMBER[(min(i, j), max(i, j))]


def kernel(
    prop, back, sink_in, origin_in, momenta_in, gtab_in, out,
    sv, hv, inbox, stream, outbox, sig, hsum, ssum, macc, kbuf, ph_hi, ph_lo,
    mom, acc, cbuf, rx, words, sink, origin, momenta, gtab,
    s_sem, h_sem, send_sem, recv_sem, ex_send, ex_recv, small_sem,
):
    ta = lax.axis_index("ta")
    gz = lax.axis_index("gz")
    cy, cx, cz = ta // 16, (ta // 4) % 4, ta % 4

    def load(src, dst, sem, c):
        sites = 1024 if c < CHUNKS - 1 else 768
        return pltpu.make_async_copy(
            src.at[:, :, :, :, pl.ds(1024 * c, sites)],
            dst.at[c, :, :, :, :, pl.ds(0, sites)],
            sem.at[c],
        )

    small = [
        pltpu.make_async_copy(src, dst, small_sem.at[i])
        for i, (src, dst) in enumerate(
            ((sink_in, sink), (origin_in, origin), (momenta_in, momenta), (gtab_in, gtab))
        )
    ]
    for copy in small:
        copy.start()
    for c in range(CHUNKS):
        load(prop, sv, s_sem, c).start()
        load(back, hv, h_sem, c).start()

    def neighbour(d):
        x, y, z = STEPS[d]
        return ((cy + y + 4) % 4 * 4 + (cx + x + 4) % 4) * 4 + (cz + z + 4) % 4

    barrier = pltpu.get_barrier_semaphore()
    for d in range(6):
        pl.semaphore_signal(barrier, inc=1, device_id=(neighbour(d), gz), device_id_type=MESH)
    pl.semaphore_signal(barrier, inc=1, device_id=(ta, 1 - gz), device_id_type=MESH)

    for n, word in enumerate(tree_words().tolist()):
        words[n] = jnp.int32(word)
    small[0].wait()
    root = sink[0]
    rel_x = (cx - root // 4 % 4 + 4) % 4
    rel_y = (cy - root // 16 + 4) % 4
    rel_z = (cz - root % 4 + 4) % 4
    rel = (rel_x * 4 + rel_y) * 4 + rel_z
    is_root = rel == 0
    into_word, from_word, depth_word = words[rel], words[64 + rel], words[128 + rel]
    into = [(into_word >> (3 * k)) & 7 for k in range(6)]
    out_of = [(from_word >> (3 * d)) & 7 for d in range(6)]
    depth = [(depth_word >> (3 * k)) & 7 for k in range(6)]

    def source(c, part):
        lo, hi = ((0, 4), (4, 7), (7, 10), (10, 13))[part]
        for k in range(6):
            for n in range(lo, hi):
                i, j = PAIRS[6 * n + k]
                re = im = None
                for m in range(12):
                    a, b = sv[c, 0, i, m], sv[c, 1, i, m]
                    if i == j:
                        r, q = a * a - b * b, a * b
                        q = q + q
                    else:
                        e, f = sv[c, 0, j, m], sv[c, 1, j, m]
                        r, q = a * e - b * f, a * f + b * e
                    re = r if re is None else re + r
                    im = q if im is None else im + q
                at = OWN + 26 * CHUNKS * k + 26 * c + 2 * n
                stream[at] = re
                stream[at + 1] = im

    def phases(chunk, pairs):
        lane = lax.broadcasted_iota(jnp.int32, (32, 128), 1).astype(F32)
        ox, oy, oz = (origin[i].astype(F32) for i in range(3))
        px, py, pz = mom[0], mom[1], mom[2]
        start = (gz * 6912 + chunk * 1024).astype(F32)
        for pair in pairs:
            for half in range(2):
                site = lane[0:8] + (start + (256.0 * pair + 128.0 * half))
                z = jnp.floor((site + 0.5) * (1.0 / 576.0))
                rest = site - z * 576.0
                x = jnp.floor((rest + 0.5) * (1.0 / 24.0))
                y = rest - x * 24.0
                x, y, z = (jnp.concatenate([v] * 4, axis=0) for v in (x - ox, y - oy, z - oz))
                wave = px * x + py * y + pz * z
                wave = wave - 24.0 * jnp.floor(wave * (1.0 / 24.0) + 0.5)
                angle = wave * (math.pi / L)
                square = angle * angle
                s = c = None
                for n in range(13, 0, -2):
                    term = (-1.0) ** (n // 2) / math.factorial(n)
                    s = term if s is None else s * square + term
                for n in range(12, -1, -2):
                    term = (-1.0) ** (n // 2) / math.factorial(n)
                    c = term if c is None else c * square + term
                s = s * angle
                twice = s + s
                for row, value in ((0, 1.0 - twice * s), (32, -(twice * c))):
                    hi = value.astype(jnp.bfloat16)
                    at = (chunk + 1, pair, pl.ds(row, 32), pl.ds(128 * half, 128))
                    ph_hi[at] = hi
                    ph_lo[at] = (value - hi.astype(F32)).astype(jnp.bfloat16)

    def sums(c, src, dst):
        for i in range(12):
            for m in range(12):
                dst[c, i, m] = src[c, 0, i, m] + src[c, 1, i, m]

    def unpack(c, block, base):
        first, last = ((0, 6), (6, 10), (10, 13))[block]
        for n in range(first, last):
            for k in range(6):
                at = base[k] + c * 26 + 2 * n
                sig[6 * n + k] = stream[at] + stream[at + 1]

    def plus(x, y):
        return y if x is None else x + y

    def contract(c, block, base):
        columns = range(3 * block, 3 * block + 3)

        def one(al):
            part = {(a, m): [None] * 3 for a in range(3) for m in columns}
            for k in range(12):
                rows = [3 * al + a for a in range(3)]
                left = [(hv[c, 0, r, k], hv[c, 1, r, k], hsum[c, r, k]) for r in rows]
                for m in columns:
                    n = pair_number(k, m)
                    at = base[n % 6] + c * 26 + n // 6 * 2
                    right = (stream[at], stream[at + 1], sig[n])
                    for a in range(3):
                        for t in range(3):
                            part[a, m][t] = plus(part[a, m][t], left[a][t] * right[t])
            total = [[None] * 3 for _ in range(4)]
            for a in range(3):
                for m in columns:
                    p1, p2, p3 = part[a, m]
                    br, bi = p1 - p2, p3 - (p1 + p2)
                    bound = (br, bi, br - bi)
                    for be in range(4):
                        row = 3 * be + a
                        forward = (sv[c, 0, row, m], sv[c, 1, row, m], ssum[c, row, m])
                        for t in range(3):
                            total[be][t] = plus(total[be][t], forward[t] * bound[t])
            for be in range(4):
                for t in range(3):
                    value = total[be][t]
                    macc[t, be, al] = value if block == 0 else macc[t, be, al] + value

        for al in range(4):
            one(al)

    def add(p, q):
        return (p[0] + q[0], p[1] + q[1])

    def sub(p, q):
        return (p[0] - q[0], p[1] - q[1])

    def pauli(m):
        d = sub(m[0][1], m[1][0])
        return [add(m[0][0], m[1][1]), add(m[1][0], m[0][1]), (-d[1], d[0]), sub(m[0][0], m[1][1])]

    def entry(be, al):
        m0, m1, m2 = macc[0, be, al], macc[1, be, al], macc[2, be, al]
        return (m0 + m1, m2 - (m0 - m1))

    def project(c):
        inner = [
            [
                pauli(
                    [
                        [
                            entry(2 * b1 + b0, 2 * a1 + a0)
                            for a0 in range(2)
                        ]
                        for b0 in range(2)
                    ]
                )
                for a1 in range(2)
            ]
            for b1 in range(2)
        ]
        site = lax.broadcasted_iota(jnp.int32, (1, 1024), 1)
        valid = (site < 768) | (c < CHUNKS - 1)
        for low in range(4):
            outer = pauli([[inner[b1][a1][low] for a1 in range(2)] for b1 in range(2)])
            for high in range(4):
                n = 4 * high + low
                for part in range(2):
                    kbuf[pl.ds(16 * part + n, 1), :] = jnp.where(valid, outer[high][part], 0.0)
        result = acc[...]
        dims = (((1,), (1,)), ((), ()))
        for pair in range(4):
            left = kbuf[:, pl.ds(256 * pair, 256)]
            hi = left.astype(jnp.bfloat16)
            lo = (left - hi.astype(F32)).astype(jnp.bfloat16)
            both = jnp.concatenate([hi, lo], axis=0)
            main = lax.dot_general(both, ph_hi[c + 1, pair], dims, preferred_element_type=F32)
            rest = lax.dot_general(hi, ph_lo[c + 1, pair], dims, preferred_element_type=F32)
            result = result + (main[0:32] + main[32:64] + rest)
        acc[...] = result

    acc[...] = jnp.zeros_like(acc)
    macc[...] = jnp.zeros_like(macc)
    ph_hi[0] = jnp.zeros((4, 64, 256), jnp.bfloat16)
    ph_lo[0] = jnp.zeros((4, 64, 256), jnp.bfloat16)
    for copy in small[1:]:
        copy.wait()
    mom[...] = jnp.zeros_like(mom)
    for p in range(NP):
        for i in range(3):
            mom[i, pl.ds(p, 1), :] = jnp.full((1, 128), momenta[i, p], jnp.int32).astype(F32)
    load(prop, sv, s_sem, 0).wait()
    source(0, 0)
    pl.semaphore_wait(barrier, 7)

    lag = LAG - 2 * gz
    shift = 13 * LAG // 2 - 13 * gz
    base = [
        jnp.where(is_root, OWN + 26 * CHUNKS * k, LINE * into[k] + depth[k] * shift)
        for k in range(6)
    ]
    line = [sum(jnp.where(out_of[d] == k, LINE * into[k], 0) for k in range(6)) for d in range(6)]
    own_line = [
        jnp.where(is_root, OWN + 26 * CHUNKS * TREE_STEPS.index(d), line[d]) for d in range(6)
    ]

    def message(s, ring, tiles, d=None):
        links = pl.ds(0, 6) if d is None else d
        return pltpu.make_async_remote_copy(
            src_ref=outbox.at[ring, links, pl.ds(0, tiles)],
            dst_ref=inbox.at[s + lag, links, pl.ds(0, tiles)],
            send_sem=send_sem.at[ring],
            recv_sem=recv_sem.at[s + lag],
            device_id=(neighbour(d or 0), gz),
            device_id_type=MESH,
        )

    def arrive(s, ring, tiles, flat):
        message(s - lag, ring, tiles).wait_recv()
        for d in range(6):
            for i in range(tiles):
                stream[LINE * d + flat + i] = inbox[s, d, i]

    def send(s, ring, tiles, flat, first_slots=False):
        if first_slots:
            pl.when(s >= OUT_RING)(message(s - OUT_RING, ring, tiles).wait_send)
        else:
            message(s - OUT_RING, ring, tiles).wait_send()
        at = own_line if first_slots else line
        for d in range(6):
            for i in range(tiles):
                outbox[ring, d, i] = stream[at[d] + flat + i]
        for d in range(6):
            message(s, ring, tiles, d).start()

    @pl.loop(0, CHUNKS)
    def _(g):
        for u in range(4):
            s = 4 * g + u
            slot = (s, u, 7 - u % 2, 26 * g + 13 * (u // 2) + 7 * (u % 2))
            pl.when(s >= lag)(functools.partial(arrive, *slot))
            send(*slot, first_slots=True)
            if u < 3:
                source(g, u + 1)
            else:
                @pl.when(g < CHUNKS - 1)
                def _():
                    for c in range(1, CHUNKS):
                        @pl.when(g + 1 == c)
                        def _(c=c):
                            load(prop, sv, s_sem, c).wait()

                    source(g + 1, 0)
            if u == 2:
                for c in range(CHUNKS):
                    @pl.when(g == c)
                    def _(c=c):
                        load(back, hv, h_sem, c).wait()

            if u % 2 == 0:
                sums(g, *((sv, ssum), (hv, hsum))[u // 2])
            else:
                phases(g, (u - 1, u))

    slot = (PACKETS, 0, 7, PACKETS // 2 * 13)
    arrive(*slot)
    send(*slot)

    @pl.loop(0, DEPTH - DEPTH * gz)
    def _(p):
        for odd in (1, 0):
            s = PACKETS + 2 * p + 2 - odd
            slot = (s, s % OUT_RING, 7 - odd, (PACKETS // 2 + p + 1 - odd) * 13 + 7 * odd)
            arrive(*slot)
            send(*slot)

    @pl.loop(0, CHUNKS)
    def _(c):
        for block in range(4):
            s = DEPTH * lag + 1 + 4 * c + block
            u = (3 + block) % 4
            ring = u + 2 * gz if u < 2 else u - 2 * gz
            odd = u % 2
            pair = DEPTH * LAG // 2 - DEPTH * gz + 2 * c + (1 + block) // 2
            slot = (s, ring, 7 - odd, 13 * pair + 7 * odd)
            pl.when(4 * c + block < PACKETS - 1)(functools.partial(arrive, *slot))
            pl.when(4 * c + block < PACKETS - 1 - lag)(functools.partial(send, *slot))
            if block == 0:
                project(c - 1)
            if block < 3:
                unpack(c, block, base)
            contract(c, block, base)

    project(CHUNKS - 1)
    for ring in range(4):
        s = PACKETS + (DEPTH - 1) * lag - 4 + ring
        message(s, ring, 7 - ring % 2).wait_send()

    swap = pltpu.make_async_remote_copy(
        src_ref=acc,
        dst_ref=rx,
        send_sem=ex_send,
        recv_sem=ex_recv,
        device_id=(ta, 1 - gz),
        device_id_type=MESH,
    )
    swap.start()
    swap.wait()
    scale = 0.125 / (72.0 * math.sqrt(L * L * L))
    value = (acc[...] + rx[...]) * scale
    kr, ki = value[0:16], value[16:32]
    cbuf[0, :, 0:32] = kr[:, 0:32] - ki[:, 32:64]
    cbuf[1, :, 0:32] = kr[:, 32:64] + ki[:, 0:32]
    for row in range(NG // 2):
        g = gtab[NG // 2 * gz + row]
        for part in range(2):
            out[part, 0, pl.ds(row, 1), :] = cbuf[part, pl.ds(g, 1), 0:NP]


def body(propagator, backward, sink_time, source_position, momenta, gamma_table):
    vmem, smem = pltpu.VMEM, pltpu.SMEM
    tile = (1, 1024)
    return pl.pallas_call(
        kernel,
        out_shape=pltpu.VMEM((2, 1, 8, NP), F32),
        in_specs=[pl.BlockSpec(memory_space=pl.ANY)] * 6,
        out_specs=pl.BlockSpec(memory_space=vmem),
        scratch_shapes=[
            vmem((CHUNKS, 2, 12, 12) + tile, F32),
            vmem((CHUNKS, 2, 12, 12) + tile, F32),
            vmem((MOST_SLOTS, 6, 7) + tile, F32),
            vmem((OWN + 6 * 26 * CHUNKS,) + tile, F32),
            vmem((OUT_RING, 6, 7) + tile, F32),
            vmem((78,) + tile, F32),
            vmem((CHUNKS, 12, 12) + tile, F32),
            vmem((CHUNKS, 12, 12) + tile, F32),
            vmem((3, 4, 4) + tile, F32),
            vmem((32, 1024), F32),
            vmem((CHUNKS + 1, 4, 64, 256), jnp.bfloat16),
            vmem((CHUNKS + 1, 4, 64, 256), jnp.bfloat16),
            vmem((3, 32, 128), F32),
            vmem((32, 64), F32),
            vmem((2, 16, 128), F32),
            vmem((32, 64), F32),
            smem((192,), jnp.int32),
            smem((1,), jnp.int32),
            smem((3,), jnp.int32),
            smem((3, NP), jnp.int32),
            smem((NG,), jnp.int32),
            pltpu.SemaphoreType.DMA((CHUNKS,)),
            pltpu.SemaphoreType.DMA((CHUNKS,)),
            pltpu.SemaphoreType.DMA((OUT_RING,)),
            pltpu.SemaphoreType.DMA((MOST_SLOTS,)),
            pltpu.SemaphoreType.DMA,
            pltpu.SemaphoreType.DMA,
            pltpu.SemaphoreType.DMA((4,)),
        ],
        compiler_params=pltpu.CompilerParams(
            collective_id=0, has_side_effects=True, vmem_limit_bytes=62_000_000
        ),
    )(
        propagator,
        backward,
        sink_time,
        source_position,
        jnp.transpose(momenta),
        gamma_table,
    )


def solution(mesh):
    in_specs = (
        P(None, None, None, "ta", "gz"),
        P(None, None, None, "ta", "gz"),
        P(),
        P(),
        P(),
        P(),
    )
    out_specs = P(None, "ta", "gz", None)
    return jax.shard_map(body, mesh=mesh, in_specs=in_specs, out_specs=out_specs, check_vma=False)
```

```python
import functools
import itertools
import math

import jax
import jax.numpy as jnp
import numpy as np
from jax import lax
from jax.experimental import pallas as pl
from jax.experimental.pallas import tpu as pltpu
from jax.sharding import PartitionSpec as P

L = 24
NG = 16
NP = 27
CHUNKS = 7
LAG = 6
PACKETS = 4 * CHUNKS
DEPTH = 7
MOST_SLOTS = PACKETS + DEPTH * LAG
LINE = MOST_SLOTS // 2 * 13
OWN = 6 * LINE
OUT_RING = 4
STEPS = ((1, 0, 0), (-1, 0, 0), (0, 1, 0), (0, -1, 0), (0, 0, 1), (0, 0, -1))
TREE_STEPS = (0, 3, 4, 1, 2, 5)
MESH = pl.DeviceIdType.MESH
F32 = jnp.float32


def moved(v, step, sign=1):
    return tuple((a + sign * b) % 4 for a, b in zip(v, step))


def turned(v):
    return tuple((-c) % 4 for c in (v[2], v[0], v[1]))


def turned_step(d):
    return tuple(-c for c in (d[2], d[0], d[1]))


@functools.cache
def tree_words():
    nodes = list(itertools.product(range(4), repeat=3))
    root, child = (0, 0, 0), (1, 0, 0)

    def level(v):
        return sum(min((a - b) % 4, (b - a) % 4) for a, b in zip(v, child))

    def orbit(tail, step):
        while step != (1, 0, 0):
            tail, step = turned(tail), turned_step(step)
        return tail

    taken = orbit(root, (1, 0, 0))
    options = {
        v: [
            (orbit(moved(v, d, -1), d), d)
            for d in STEPS
            if moved(v, d, -1) != root and level(moved(v, d, -1)) < level(v)
        ]
        for v in nodes
        if v not in (root, child)
    }
    match = {}

    def augment(v, seen):
        for key, d in options[v]:
            if key == taken or key in seen:
                continue
            seen.add(key)
            if key not in match or augment(match[key][0], seen):
                match[key] = (v, d)
                return True
        return False

    for v in options:
        assert augment(v, set())
    into = {child: (1, 0, 0)}
    for v, d in match.values():
        into[v] = d
    depth = {root: 0}

    def depth_of(v):
        if v not in depth:
            depth[v] = depth_of(moved(v, into[v], -1)) + 1
        return depth[v]

    edges = [(v, d) for v, d in into.items()]
    depths = {v: depth_of(v) for v in nodes}
    words = np.zeros((3, 64), np.int32)

    def number(v):
        return (v[0] * 4 + v[1]) * 4 + v[2]

    seen_edges = set()
    for k in range(6):
        assert STEPS.index([d for v, d in edges if moved(v, d, -1) == root][0]) == TREE_STEPS[k]
        for v, d in edges:
            n, j = number(v), STEPS.index(d)
            tail = number(moved(v, d, -1))
            assert (tail, j) not in seen_edges
            seen_edges.add((tail, j))
            words[0, n] |= j << (3 * k)
            words[1, tail] |= k << (3 * j)
        for v, n_hops in depths.items():
            assert n_hops <= DEPTH
            words[2, number(v)] |= n_hops << (3 * k)
        edges = [(turned(v), turned_step(d)) for v, d in edges]
        depths = {turned(v): n_hops for v, n_hops in depths.items()}
    return words.reshape(-1)


PAIRS = [(i, j) for i in range(12) for j in range(i, 12)]
PAIR_NUMBER = {p: n for n, p in enumerate(PAIRS)}


def pair_number(i, j):
    return PAIR_NUMBER[(min(i, j), max(i, j))]


def kernel(
    prop, back, sink_in, origin_in, momenta_in, gtab_in, out,
    sv, hv, inbox, stream, outbox, sig, hsum, ssum, macc, kbuf, ph_hi, ph_lo,
    mom, acc, cbuf, rx, words, sink, origin, momenta, gtab,
    s_sem, h_sem, send_sem, recv_sem, ex_send, ex_recv, small_sem,
):
    ta = lax.axis_index("ta")
    gz = lax.axis_index("gz")
    cy, cx, cz = ta // 16, (ta // 4) % 4, ta % 4

    def load(src, dst, sem, c):
        sites = 1024 if c < CHUNKS - 1 else 768
        return pltpu.make_async_copy(
            src.at[:, :, :, :, pl.ds(1024 * c, sites)],
            dst.at[c, :, :, :, :, pl.ds(0, sites)],
            sem.at[c],
        )

    small = [
        pltpu.make_async_copy(src, dst, small_sem.at[i])
        for i, (src, dst) in enumerate(
            ((sink_in, sink), (origin_in, origin), (momenta_in, momenta), (gtab_in, gtab))
        )
    ]
    for copy in small:
        copy.start()
    for c in range(CHUNKS):
        load(prop, sv, s_sem, c).start()
        load(back, hv, h_sem, c).start()

    def neighbour(d):
        x, y, z = STEPS[d]
        return ((cy + y + 4) % 4 * 4 + (cx + x + 4) % 4) * 4 + (cz + z + 4) % 4

    barrier = pltpu.get_barrier_semaphore()
    for d in range(6):
        pl.semaphore_signal(barrier, inc=1, device_id=(neighbour(d), gz), device_id_type=MESH)
    pl.semaphore_signal(barrier, inc=1, device_id=(ta, 1 - gz), device_id_type=MESH)

    for n, word in enumerate(tree_words().tolist()):
        words[n] = jnp.int32(word)
    small[0].wait()
    root = sink[0]
    rel_x = (cx - root // 4 % 4 + 4) % 4
    rel_y = (cy - root // 16 + 4) % 4
    rel_z = (cz - root % 4 + 4) % 4
    rel = (rel_x * 4 + rel_y) * 4 + rel_z
    is_root = rel == 0
    into_word, from_word, depth_word = words[rel], words[64 + rel], words[128 + rel]
    into = [(into_word >> (3 * k)) & 7 for k in range(6)]
    out_of = [(from_word >> (3 * d)) & 7 for d in range(6)]
    depth = [(depth_word >> (3 * k)) & 7 for k in range(6)]

    def source(c, part):
        lo, hi = ((0, 4), (4, 7), (7, 10), (10, 13))[part]
        for k in range(6):
            for n in range(lo, hi):
                i, j = PAIRS[6 * n + k]
                re = im = None
                for m in range(12):
                    a, b = sv[c, 0, i, m], sv[c, 1, i, m]
                    if i == j:
                        r, q = a * a - b * b, a * b
                        q = q + q
                    else:
                        e, f = sv[c, 0, j, m], sv[c, 1, j, m]
                        r, q = a * e - b * f, a * f + b * e
                    re = r if re is None else re + r
                    im = q if im is None else im + q
                at = OWN + 26 * CHUNKS * k + 26 * c + 2 * n
                stream[at] = re
                stream[at + 1] = im

    def phases(chunk, pairs):
        lane = lax.broadcasted_iota(jnp.int32, (32, 128), 1).astype(F32)
        ox, oy, oz = (origin[i].astype(F32) for i in range(3))
        px, py, pz = mom[0], mom[1], mom[2]
        start = (gz * 6912 + chunk * 1024).astype(F32)
        for pair in pairs:
            for half in range(2):
                site = lane[0:8] + (start + (256.0 * pair + 128.0 * half))
                z = jnp.floor((site + 0.5) * (1.0 / 576.0))
                rest = site - z * 576.0
                x = jnp.floor((rest + 0.5) * (1.0 / 24.0))
                y = rest - x * 24.0
                x, y, z = (jnp.concatenate([v] * 4, axis=0) for v in (x - ox, y - oy, z - oz))
                wave = px * x + py * y + pz * z
                wave = wave - 24.0 * jnp.floor(wave * (1.0 / 24.0) + 0.5)
                angle = wave * (math.pi / L)
                square = angle * angle
                s = c = None
                for n in range(13, 0, -2):
                    term = (-1.0) ** (n // 2) / math.factorial(n)
                    s = term if s is None else s * square + term
                for n in range(12, -1, -2):
                    term = (-1.0) ** (n // 2) / math.factorial(n)
                    c = term if c is None else c * square + term
                s = s * angle
                twice = s + s
                for row, value in ((0, 1.0 - twice * s), (32, -(twice * c))):
                    hi = value.astype(jnp.bfloat16)
                    at = (chunk + 1, pair, pl.ds(row, 32), pl.ds(128 * half, 128))
                    ph_hi[at] = hi
                    ph_lo[at] = (value - hi.astype(F32)).astype(jnp.bfloat16)

    def sums(c, src, dst):
        for i in range(12):
            for m in range(12):
                dst[c, i, m] = src[c, 0, i, m] + src[c, 1, i, m]

    def unpack(c, block, base):
        first, last = ((0, 6), (6, 10), (10, 13))[block]
        for n in range(first, last):
            for k in range(6):
                at = base[k] + c * 26 + 2 * n
                sig[6 * n + k] = stream[at] + stream[at + 1]

    def plus(x, y):
        return y if x is None else x + y

    def contract(c, block, base):
        columns = range(3 * block, 3 * block + 3)

        def one(al):
            part = {(a, m): [None] * 3 for a in range(3) for m in columns}
            for k in range(12):
                rows = [3 * al + a for a in range(3)]
                left = [(hv[c, 0, r, k], hv[c, 1, r, k], hsum[c, r, k]) for r in rows]
                for m in columns:
                    n = pair_number(k, m)
                    at = base[n % 6] + c * 26 + n // 6 * 2
                    right = (stream[at], stream[at + 1], sig[n])
                    for a in range(3):
                        for t in range(3):
                            part[a, m][t] = plus(part[a, m][t], left[a][t] * right[t])
            total = [[None] * 3 for _ in range(4)]
            for a in range(3):
                for m in columns:
                    p1, p2, p3 = part[a, m]
                    br, bi = p1 - p2, p3 - (p1 + p2)
                    bound = (br, bi, br - bi)
                    for be in range(4):
                        row = 3 * be + a
                        forward = (sv[c, 0, row, m], sv[c, 1, row, m], ssum[c, row, m])
                        for t in range(3):
                            total[be][t] = plus(total[be][t], forward[t] * bound[t])
            for be in range(4):
                for t in range(3):
                    value = total[be][t]
                    macc[t, be, al] = value if block == 0 else macc[t, be, al] + value

        for al in range(4):
            one(al)

    def add(p, q):
        return (p[0] + q[0], p[1] + q[1])

    def sub(p, q):
        return (p[0] - q[0], p[1] - q[1])

    def pauli(m):
        d = sub(m[0][1], m[1][0])
        return [add(m[0][0], m[1][1]), add(m[1][0], m[0][1]), (-d[1], d[0]), sub(m[0][0], m[1][1])]

    def entry(be, al):
        m0, m1, m2 = macc[0, be, al], macc[1, be, al], macc[2, be, al]
        return (m0 + m1, m2 - (m0 - m1))

    def project(c):
        inner = [
            [
                pauli(
                    [
                        [
                            entry(2 * b1 + b0, 2 * a1 + a0)
                            for a0 in range(2)
                        ]
                        for b0 in range(2)
                    ]
                )
                for a1 in range(2)
            ]
            for b1 in range(2)
        ]
        site = lax.broadcasted_iota(jnp.int32, (1, 1024), 1)
        valid = (site < 768) | (c < CHUNKS - 1)
        for low in range(4):
            outer = pauli([[inner[b1][a1][low] for a1 in range(2)] for b1 in range(2)])
            for high in range(4):
                n = 4 * high + low
                for part in range(2):
                    kbuf[pl.ds(16 * part + n, 1), :] = jnp.where(valid, outer[high][part], 0.0)
        result = acc[...]
        dims = (((1,), (1,)), ((), ()))
        for pair in range(4):
            left = kbuf[:, pl.ds(256 * pair, 256)]
            hi = left.astype(jnp.bfloat16)
            lo = (left - hi.astype(F32)).astype(jnp.bfloat16)
            both = jnp.concatenate([hi, lo], axis=0)
            main = lax.dot_general(both, ph_hi[c + 1, pair], dims, preferred_element_type=F32)
            rest = lax.dot_general(hi, ph_lo[c + 1, pair], dims, preferred_element_type=F32)
            result = result + (main[0:32] + main[32:64] + rest)
        acc[...] = result

    def prepare():
        acc[...] = jnp.zeros_like(acc)
        macc[...] = jnp.zeros_like(macc)
        ph_hi[0] = jnp.zeros((4, 64, 256), jnp.bfloat16)
        ph_lo[0] = jnp.zeros((4, 64, 256), jnp.bfloat16)
        for copy in small[1:]:
            copy.wait()
        mom[...] = jnp.zeros_like(mom)
        for p in range(NP):
            for i in range(3):
                mom[i, pl.ds(p, 1), :] = jnp.full((1, 128), momenta[i, p], jnp.int32).astype(F32)

    load(prop, sv, s_sem, 0).wait()
    source(0, 0)
    pl.semaphore_wait(barrier, 7)

    lag = LAG - 2 * gz
    shift = 13 * LAG // 2 - 13 * gz
    base = [
        jnp.where(is_root, OWN + 26 * CHUNKS * k, LINE * into[k] + depth[k] * shift)
        for k in range(6)
    ]
    line = [sum(jnp.where(out_of[d] == k, LINE * into[k], 0) for k in range(6)) for d in range(6)]
    own_line = [
        jnp.where(is_root, OWN + 26 * CHUNKS * TREE_STEPS.index(d), line[d]) for d in range(6)
    ]

    def message(s, ring, tiles, d=None):
        links = pl.ds(0, 6) if d is None else d
        return pltpu.make_async_remote_copy(
            src_ref=outbox.at[ring, links, pl.ds(0, tiles)],
            dst_ref=inbox.at[s + lag, links, pl.ds(0, tiles)],
            send_sem=send_sem.at[ring],
            recv_sem=recv_sem.at[s + lag],
            device_id=(neighbour(d or 0), gz),
            device_id_type=MESH,
        )

    def arrive(s, ring, tiles, flat):
        message(s - lag, ring, tiles).wait_recv()
        for d in range(6):
            for i in range(tiles):
                stream[LINE * d + flat + i] = inbox[s, d, i]

    def send(s, ring, tiles, flat, first_slots=False):
        if first_slots:
            pl.when(s >= OUT_RING)(message(s - OUT_RING, ring, tiles).wait_send)
        else:
            message(s - OUT_RING, ring, tiles).wait_send()
        at = own_line if first_slots else line
        for d in range(6):
            for i in range(tiles):
                outbox[ring, d, i] = stream[at[d] + flat + i]
        for d in range(6):
            message(s, ring, tiles, d).start()

    @pl.loop(0, CHUNKS)
    def _(g):
        for u in range(4):
            s = 4 * g + u
            slot = (s, u, 7 - u % 2, 26 * g + 13 * (u // 2) + 7 * (u % 2))
            pl.when(s >= lag)(functools.partial(arrive, *slot))
            send(*slot, first_slots=True)
            if u == 0:
                pl.when(g == 0)(prepare)
            if u < 3:
                source(g, u + 1)
            else:
                @pl.when(g < CHUNKS - 1)
                def _():
                    for c in range(1, CHUNKS):
                        @pl.when(g + 1 == c)
                        def _(c=c):
                            load(prop, sv, s_sem, c).wait()

                    source(g + 1, 0)
            if u == 2:
                for c in range(CHUNKS):
                    @pl.when(g == c)
                    def _(c=c):
                        load(back, hv, h_sem, c).wait()

            if u % 2 == 0:
                sums(g, *((sv, ssum), (hv, hsum))[u // 2])
            else:
                phases(g, (u - 1, u))

    slot = (PACKETS, 0, 7, PACKETS // 2 * 13)
    arrive(*slot)
    send(*slot)

    @pl.loop(0, DEPTH - DEPTH * gz)
    def _(p):
        for odd in (1, 0):
            s = PACKETS + 2 * p + 2 - odd
            slot = (s, s % OUT_RING, 7 - odd, (PACKETS // 2 + p + 1 - odd) * 13 + 7 * odd)
            arrive(*slot)
            send(*slot)

    @pl.loop(0, CHUNKS)
    def _(c):
        for block in range(4):
            s = DEPTH * lag + 1 + 4 * c + block
            u = (3 + block) % 4
            ring = u + 2 * gz if u < 2 else u - 2 * gz
            odd = u % 2
            pair = DEPTH * LAG // 2 - DEPTH * gz + 2 * c + (1 + block) // 2
            slot = (s, ring, 7 - odd, 13 * pair + 7 * odd)
            pl.when(4 * c + block < PACKETS - 1)(functools.partial(arrive, *slot))
            pl.when(4 * c + block < PACKETS - 1 - lag)(functools.partial(send, *slot))
            if block == 0:
                project(c - 1)
            if block < 3:
                unpack(c, block, base)
            contract(c, block, base)

    project(CHUNKS - 1)
    for ring in range(4):
        s = PACKETS + (DEPTH - 1) * lag - 4 + ring
        message(s, ring, 7 - ring % 2).wait_send()

    swap = pltpu.make_async_remote_copy(
        src_ref=acc,
        dst_ref=rx,
        send_sem=ex_send,
        recv_sem=ex_recv,
        device_id=(ta, 1 - gz),
        device_id_type=MESH,
    )
    swap.start()
    swap.wait()
    scale = 0.125 / (72.0 * math.sqrt(L * L * L))
    value = (acc[...] + rx[...]) * scale
    kr, ki = value[0:16], value[16:32]
    cbuf[0, :, 0:32] = kr[:, 0:32] - ki[:, 32:64]
    cbuf[1, :, 0:32] = kr[:, 32:64] + ki[:, 0:32]
    for row in range(NG // 2):
        g = gtab[NG // 2 * gz + row]
        for part in range(2):
            out[part, 0, pl.ds(row, 1), :] = cbuf[part, pl.ds(g, 1), 0:NP]


def body(propagator, backward, sink_time, source_position, momenta, gamma_table):
    vmem, smem = pltpu.VMEM, pltpu.SMEM
    tile = (1, 1024)
    return pl.pallas_call(
        kernel,
        out_shape=pltpu.VMEM((2, 1, 8, NP), F32),
        in_specs=[pl.BlockSpec(memory_space=pl.ANY)] * 6,
        out_specs=pl.BlockSpec(memory_space=vmem),
        scratch_shapes=[
            vmem((CHUNKS, 2, 12, 12) + tile, F32),
            vmem((CHUNKS, 2, 12, 12) + tile, F32),
            vmem((MOST_SLOTS, 6, 7) + tile, F32),
            vmem((OWN + 6 * 26 * CHUNKS,) + tile, F32),
            vmem((OUT_RING, 6, 7) + tile, F32),
            vmem((78,) + tile, F32),
            vmem((CHUNKS, 12, 12) + tile, F32),
            vmem((CHUNKS, 12, 12) + tile, F32),
            vmem((3, 4, 4) + tile, F32),
            vmem((32, 1024), F32),
            vmem((CHUNKS + 1, 4, 64, 256), jnp.bfloat16),
            vmem((CHUNKS + 1, 4, 64, 256), jnp.bfloat16),
            vmem((3, 32, 128), F32),
            vmem((32, 64), F32),
            vmem((2, 16, 128), F32),
            vmem((32, 64), F32),
            smem((192,), jnp.int32),
            smem((1,), jnp.int32),
            smem((3,), jnp.int32),
            smem((3, NP), jnp.int32),
            smem((NG,), jnp.int32),
            pltpu.SemaphoreType.DMA((CHUNKS,)),
            pltpu.SemaphoreType.DMA((CHUNKS,)),
            pltpu.SemaphoreType.DMA((OUT_RING,)),
            pltpu.SemaphoreType.DMA((MOST_SLOTS,)),
            pltpu.SemaphoreType.DMA,
            pltpu.SemaphoreType.DMA,
            pltpu.SemaphoreType.DMA((4,)),
        ],
        compiler_params=pltpu.CompilerParams(
            collective_id=0, has_side_effects=True, vmem_limit_bytes=62_000_000
        ),
    )(
        propagator,
        backward,
        sink_time,
        source_position,
        jnp.transpose(momenta),
        gamma_table,
    )


def solution(mesh):
    in_specs = (
        P(None, None, None, "ta", "gz"),
        P(None, None, None, "ta", "gz"),
        P(),
        P(),
        P(),
        P(),
    )
    out_specs = P(None, "ta", "gz", None)
    return jax.shard_map(body, mesh=mesh, in_specs=in_specs, out_specs=out_specs, check_vma=False)
```
